256 devices in a mesh: ens: 2 (over y), gx: 128 (over x, z, core).
Axes of the slice: x: 4, y: 2, z: 16, core: 2. Of those that a mesh axis runs over, the one named last changes fastest.
The devices are a block of a 4x16x16 slice.
Arguments:
- model_state: float32 [8, 4, 2560, 2560], P('ens', None, 'gx'), parts along dimension 0, may hold values from -6 to 6
- driving: float32 [8, 4, 2560, 2560], P('ens', None, 'gx'), parts along dimension 0, may hold values from -12 to 12
- mode_east: int32 [30], replicated, may hold values from 1 to 60, as said below
- mode_north: int32 [30], replicated, may hold values from 1 to 60, as said below
- level_class: int32 [4], replicated, may hold values from 0 to 7
- nudge_table: float32 [8, 4], replicated, may hold values from 0.05 to 0.5
Outputs:
- nudged: float32 [8, 4, 2560, 2560], P('ens', None, 'gx'), parts along dimension 0
- residual_log: float32 [8, 4], P('ens'), parts along dimension 0
The draws below stay inside these ranges and needn't reach their ends.
There are 2 independent parts, one for each index of `ens`. The reference program is written for one: setup_inputs(seed, part) draws one part's arguments, and reference() takes and returns one part's arrays. A program takes and returns all parts, laid end to end along the dimension named above; an argument that names none is the same for every part. Nothing has to cross between parts.
Inputs may be any that keep to these rules, and one draw needn't show every extreme that they name: `mode_east`: 30 distinct wavenumbers in increasing order, the first 1 and the last 60. `mode_north`: 30 distinct wavenumbers in increasing order, the first 1 and the last 60.
All inputs are finite; a program needn't handle non-finite values.
Results may differ from the reference program's by a relative error of at most 0.0001.
Values sent between devices are 32-bit elements; how exact they have to be, the bound alone decides.
A program may use at most 128 MiB of HBM per device.

```python
import math
import jax
import jax.numpy as jnp
from jax import lax

F = 4
KX = 30
KY = 30
ITERS = 4
NTAB = 8
LEV = 4
NY = 2560
NX = 2560


def pick_modes(key, offset_salt, mode_count):
    chosen = jax.random.permutation(jax.random.fold_in(key, offset_salt), 2 * mode_count - 2)[:mode_count - 2] + 2
    first_one = jnp.array([1], jnp.int32)
    last_one = jnp.array([2 * mode_count], jnp.int32)
    return jnp.sort(jnp.concatenate([first_one, chosen.astype(jnp.int32), last_one]))


def draw_mode_east(key, part):
    return pick_modes(key, 11, KX)


def draw_mode_north(key, part):
    return pick_modes(key, 23, KY)


def draw_driving(key, part):
    rough_key, amp_key = jax.random.split(jax.random.fold_in(key, 37), 2)
    full_shape = (F, LEV, NX, NY)
    east_pos = jnp.arange(NX, dtype=jnp.float32)
    north_pos = jnp.arange(NY, dtype=jnp.float32)
    rising = jnp.sqrt(1.0 + 2.0 * east_pos / max(NX - 1, 1))[None, None, :, None]
    wave_nums = jnp.arange(1, 17, dtype=jnp.float32)
    east_table = jnp.sin(jnp.pi * wave_nums[:, None] * (east_pos[None, :] + 1.0) / (NX + 1))
    north_table = jnp.sin(jnp.pi * wave_nums[:, None] * (north_pos[None, :] + 1.0) / (NY + 1))
    amplitudes = jax.random.uniform(amp_key, (F, LEV, 16, 16), jnp.float32, -0.25, 0.25)
    smooth = jnp.einsum('flab,ax,by->flxy', amplitudes, east_table, north_table)
    rough = jnp.clip(jax.random.normal(rough_key, full_shape, jnp.float32), -5.0, 5.0)
    result = rough * rising + smooth
    return jnp.clip(result, -12.0, 12.0)


def with_ends(entries, stream_key, low, top_value):
    longest = entries.shape.index(max(entries.shape))
    spots = []
    for shift in (0, 1):
        where = [jax.random.randint(jax.random.fold_in(stream_key, axis), (), 0, length) for axis, length in enumerate(entries.shape)]
        where[longest] = (where[longest] + shift) % entries.shape[longest]
        spots.append(tuple(where))
    return entries.at[spots[0]].set(low).at[spots[1]].set(top_value)


def steps_of(key, extent, pieces, least, top_value):
    def one(dim, parts):
        draws = jax.random.uniform(jax.random.fold_in(jax.random.fold_in(key, 6), dim), (parts,), jnp.float32, least / len(pieces), top_value / len(pieces))
        return jnp.repeat(jnp.exp(draws), extent[dim] // parts).reshape((-1,) + (1,) * (len(extent) - dim - 1))

    level = one(*pieces[0])
    for cut in pieces[1:]:
        level = level * one(*cut)
    return level


def centred(rng, dims, scale, most, shards=(), kind=jnp.bfloat16):
    drawn = jax.random.normal(rng, dims, jnp.float32) * scale
    if len(shards) > 0:
        drawn = steps_of(rng, dims, shards, -0.22, 0.18) * drawn
    return jnp.clip(drawn, min=-most, max=most).astype(kind)


def setup_inputs(seed: int = 0, part: int = 0) -> dict:
    seeds = jax.random.split(jax.random.key(seed), 7)
    part_keys = jax.random.split(jax.random.fold_in(seeds[6], part), 7)
    return {
        "model_state": centred(part_keys[0], (F, LEV, NX, NY), 1.0, 6.0, ((2, 128),), jnp.float32),
        "driving": draw_driving(jax.random.fold_in(jax.random.fold_in(seeds[6], part), 71), part),
        "mode_east": draw_mode_east(jax.random.fold_in(seeds[6], 71), part),
        "mode_north": draw_mode_north(jax.random.fold_in(seeds[6], 71), part),
        "level_class": with_ends(jax.random.randint(seeds[4], (LEV,), 0, NTAB), jax.random.fold_in(seeds[4], 1), 0, NTAB - 1).astype(jnp.int32),
        "nudge_table": jnp.clip(jnp.exp(jax.random.uniform(seeds[5], (NTAB, F), jnp.float32, math.log(0.05), math.log(0.5))), 0.05, 0.5),
    }


DIFFUSION = 0.24

def sine_table(wavenums, grid_cells):
    places = jnp.arange(1, grid_cells + 1, dtype=jnp.int32)
    phases = wavenums.astype(jnp.int32)[:, None] * places[None, :] % (2 * (grid_cells + 1))
    return jnp.sin(phases.astype(jnp.float32) * (jnp.pi / (grid_cells + 1)))

def reference(model_state, driving, mode_east, mode_north, level_class, nudge_table):
    fields, levels, total_east, north_cells = model_state.shape
    table_east = sine_table(mode_east, total_east)
    table_north = sine_table(mode_north, north_cells)
    weights = nudge_table[level_class].T
    scale_norm = 4.0 / ((total_east + 1) * (north_cells + 1))
    cell_count = float(levels * total_east * north_cells)
    current = model_state
    records = []
    for substep in range(ITERS):
        deviation = driving - current
        along_north = jnp.einsum('flxy,by->flxb', deviation, table_north, precision=lax.Precision.HIGHEST)
        coeffs = jnp.einsum('flxb,ax->flab', along_north, table_east, precision=lax.Precision.HIGHEST) * scale_norm
        partial_value = jnp.einsum('flab,ax->flxb', coeffs, table_east, precision=lax.Precision.HIGHEST)
        tendency = jnp.einsum('flxb,by->flxy', partial_value, table_north, precision=lax.Precision.HIGHEST)
        tendency = tendency * weights[:, :, None, None]
        padded = jnp.pad(current, ((0, 0), (0, 0), (1, 1), (1, 1)))
        stencil = padded[:, :, 2:, 1:-1] + padded[:, :, :-2, 1:-1] + padded[:, :, 1:-1, 2:] + padded[:, :, 1:-1, :-2] - 4.0 * current
        current = current + tendency + DIFFUSION * stencil
        remain = driving - current
        records.append(jnp.sqrt(lax.optimization_barrier(jnp.sum(remain * remain, axis=(1, 2, 3))) / cell_count))
    return (current, jnp.stack(records))
```

```python
import functools

import jax
import jax.numpy as jnp
import numpy as np
from jax import lax
from jax.experimental import pallas as pl
from jax.experimental.pallas import tpu as pltpu
from jax.sharding import PartitionSpec as P

ITERS = 4
DIFFUSION = 0.24
CORES = 2
RING = 16
MESH = pl.DeviceIdType.MESH
HIGHEST = lax.Precision.HIGHEST
F32 = jnp.float32
LANES = 128
HALO = 4
PAD = 8


def iota(shape, dim):
    return lax.broadcasted_iota(jnp.int32, shape, dim)


def pick(ref, which, count):
    out = jnp.zeros(which.shape, F32)
    for i in range(count):
        out = jnp.where(which == i, ref[i].astype(F32), out)
    return out


def sine(product, period):
    turns = jnp.floor(product * (1.0 / period) + 0.5)
    x = (product - turns * period) * (np.pi / period)
    odd = turns - 2.0 * jnp.floor(turns * 0.5)
    y = x * x
    poly = 1.0 / 6227020800.0
    for c in (-1.0 / 39916800.0, 1.0 / 362880.0, -1.0 / 5040.0, 1.0 / 120.0, -1.0 / 6.0, 1.0):
        poly = poly * y + c
    return x * poly * (1.0 - 2.0 * odd)


def split(value):
    high = value.astype(jnp.bfloat16)
    return high, (value - high.astype(F32)).astype(jnp.bfloat16)


def kernel(
    tiles, u_hbm, d_hbm, me_ref, mn_ref, lc_ref, nt_ref, o_hbm, res_ref,
    U, D, O, W, T, CA, RA, QB, DB, QC, SB, EB, ACC, PS,
    in_sem, out_sem, hs_sem, hr_sem, as_sem, ar_sem, qs_sem, qr_sem, ds_sem, dr_sem,
    cs_sem, cr_sem, ss_sem, sr_sem, es_sem, er_sem,
):
    fields, cols, levels, north = u_hbm.shape
    kx, ky = me_ref.shape[0], mn_ref.shape[0]
    east = cols * tiles
    members = tiles // RING
    chunks = north // LANES
    blocks = chunks // 2
    wide = cols + 2 * HALO
    rows = 8 * blocks
    high_rows = rows + 2 * PAD
    own = pl.ds(HALO, cols)
    g = lax.axis_index("gx")
    core = lax.rem(g, CORES)
    z = lax.rem(g // CORES, RING)
    xi = g // (CORES * RING)
    me = xi * CORES + core

    def member(i):
        return {"gx": ((i // CORES) * RING + z) * CORES + lax.rem(i, CORES)}

    def ring(i):
        return {"gx": (xi * RING + i) * CORES + core}

    right = {"gx": lax.rem(g + 1, tiles)}
    left = {"gx": lax.rem(g + tiles - 1, tiles)}
    others = [lax.rem(me + k, members) for k in range(1, members)]
    far_first = sorted(range(1, RING), key=lambda k: -min(k, RING - k))
    spots = [lax.rem(z + k, RING) for k in far_first]

    u_view = U.reshape(fields, wide, high_rows // levels, levels, LANES)
    d_view = D.reshape(fields, cols, chunks, levels, LANES)
    o_view = O.reshape(fields, cols, chunks, levels, LANES)
    skip = PAD // levels
    for h in range(0, fields, 2):
        for i in range(2):
            for f in (h, h + 1):
                for t in range(chunks):
                    hbm, dst = (
                        (u_hbm, u_view.at[f, own, skip + t]) if i == 0 else (d_hbm, d_view.at[f, :, t])
                    )
                    pltpu.make_async_copy(
                        hbm.at[f, :, :, pl.ds(t * LANES, LANES)], dst, in_sem.at[i, f]
                    ).start()

    def loaded(i, f):
        ref = U.at[f, own, pl.ds(PAD, rows)] if i == 0 else D.at[f]
        pltpu.make_async_copy(ref, ref, in_sem.at[i, f]).wait()

    barrier = pltpu.get_barrier_semaphore()
    greeted = [member(i) for i in others] + [ring(i) for i in spots] + [left, right]
    for who in greeted:
        pl.semaphore_signal(barrier, inc=1, device_id=who, device_id_type=MESH)

    row32 = iota((32, LANES), 0)
    lane32 = iota((32, LANES), 1)
    modes_n = pick(mn_ref, row32, ky)
    for c in range(chunks):
        place = (lane32 + (c * LANES + 1)).astype(F32)
        high, low = split(sine(modes_n * place, float(north + 1)))
        at = pl.ds(c * LANES, LANES)
        both = jnp.concatenate([high, low], axis=0)
        T[0:64, at] = both
        T[64:128, at] = both
    first = g * cols
    count = 8 * cols
    grid_rows = 8 * ((count + LANES - 1) // LANES) * (LANES // 8)
    row_m, lane_m = iota((LANES, grid_rows), 0), iota((LANES, grid_rows), 1)
    mode_m = pick(me_ref, iota((LANES, LANES), 0) % 32, kx)
    mode_m = jnp.concatenate([mode_m] * (grid_rows // LANES), axis=1)
    to_modes = jnp.where(
        (lane_m < count) & (row_m // 32 == lane_m % 4),
        sine(mode_m * (lane_m // 8 + first + 1).astype(F32), float(east + 1)), 0.0,
    )
    row_g, lane_g = iota((count, LANES), 0), iota((count, LANES), 1)
    mode_g = jnp.concatenate([pick(me_ref, iota((8, LANES), 1) % 32, kx)] * cols, axis=0)
    to_grid = jnp.where(
        row_g % 4 == lane_g // 32,
        sine(mode_g * (row_g // 8 + first + 1).astype(F32), float(east + 1)), 0.0,
    )
    edge = jnp.zeros((wide, PAD, LANES), F32)
    for f in range(fields):
        U[f, :, 0:PAD] = edge
        U[f, :, PAD + rows : high_rows] = edge
    for s in range(2):
        W[s, :, 0:PAD] = edge
        W[s, :, PAD + rows : high_rows] = edge

    row16 = iota((16, LANES), 0)
    lane16 = iota((16, LANES), 1)
    a16 = row16 + jnp.where(lane16 >= 64, 16, 0)
    b16 = lane16 % 32
    upper = lane16 % 64 >= 32
    half_e = sine(pick(me_ref, a16, kx), 2.0 * (east + 1))
    half_n = sine(pick(mn_ref, b16, ky), 2.0 * (north + 1))
    fade = (4.0 * DIFFUSION) * (half_e * half_e + half_n * half_n)
    lam = 1.0 - fade
    f_low = 2 * (me // levels)
    my_class = lc_ref[lax.rem(me, levels)]
    w16 = jnp.where(upper, nt_ref[my_class, f_low + 1], nt_ref[my_class, f_low])

    def substeps(r, d):
        t = jnp.zeros_like(r)
        v = r
        out = []
        for _ in range(ITERS):
            t = lam * t + w16 * r
            r = (lam - w16) * r + fade * d
            v = lam * v + fade * d
            out.append((t, r, v))
        return out

    norm = 4.0 / ((east + 1) * (north + 1))
    odd_chunk = row_g % 8 >= 4
    contract_lanes = (((1,), (1,)), ((), ()))
    for h in range(0, fields, 2):
        for f in (h, h + 1):
            loaded(0, f)
        for f in (h, h + 1):
            loaded(1, f)
        acc_r = acc_d = None
        held = []
        for k in range(blocks):
            at = pl.ds(8 * k, 8)
            d = D[h : h + 2, :, at]
            r = d - U[h : h + 2, own, pl.ds(PAD + 8 * k, 8)]
            high, low = split(r.reshape(2 * count, LANES))
            table = jnp.concatenate(
                [T[0:64, pl.ds((2 * k + p) * LANES, LANES)] for p in range(2)], axis=0
            )
            out = lax.dot_general(
                jnp.concatenate([high, low], axis=1), jnp.concatenate([table, table], axis=1),
                contract_lanes, preferred_element_type=F32,
            )
            acc_r = out if acc_r is None else acc_r + out
            held.append((d.reshape(2 * count, LANES).astype(jnp.bfloat16), table))
            if len(held) == 2:
                out = lax.dot_general(
                    jnp.concatenate([held[0][0], held[1][0]], axis=1),
                    jnp.concatenate([held[0][1], held[1][1]], axis=1),
                    contract_lanes, preferred_element_type=F32,
                )
                acc_d = out if acc_d is None else acc_d + out
                held = []
        mix = jnp.zeros((count, LANES), F32)
        for i, acc in enumerate((acc_r, acc_d)):
            acc = acc + pltpu.roll(acc, 32, 1)
            for j in range(2):
                mine = acc[j * count : (j + 1) * count]
                slot = 2 * i + j
                even, odd = ((slot - 1) % 4) * 32, ((slot + 1) % 4) * 32
                even = pltpu.roll(mine, even, 1) if even else mine
                odd = pltpu.roll(mine, odd, 1) if odd else mine
                mix = jnp.where(lane_g // 32 == slot, jnp.where(odd_chunk, odd, even), mix)
        if grid_rows > count:
            mix = jnp.concatenate([mix, jnp.zeros((grid_rows - count, LANES), F32)], axis=0)
        modal = norm * jnp.dot(to_modes, mix, precision=HIGHEST, preferred_element_type=F32)
        for l in range(levels):
            CA[(h // 2) * levels + l] = modal[32 * l : 32 * l + 32]

    pl.semaphore_wait(barrier, len(greeted))

    def send(src, dst, send_sem, recv_sem, who):
        copy = pltpu.make_async_remote_copy(
            src_ref=src, dst_ref=dst, send_sem=send_sem, recv_sem=recv_sem,
            device_id=who, device_id_type=MESH,
        )
        copy.start()
        return copy

    def landed(ref, sem, who):
        pltpu.make_async_remote_copy(
            src_ref=ref, dst_ref=ref, send_sem=sem, recv_sem=sem,
            device_id=who, device_id_type=MESH,
        ).wait_recv()

    sent = []
    for i in others:
        sent.append(send(CA.at[i], RA.at[me], as_sem.at[i], ar_sem.at[me], member(i)))
    body_rows = pl.ds(PAD, rows)
    for f in range(fields):
        sent.append(send(
            U.at[f, pl.ds(cols, HALO), body_rows], U.at[f, pl.ds(0, HALO), body_rows],
            hs_sem.at[0, f], hr_sem.at[0, f], right,
        ))
        sent.append(send(
            U.at[f, pl.ds(HALO, HALO), body_rows], U.at[f, pl.ds(HALO + cols, HALO), body_rows],
            hs_sem.at[1, f], hr_sem.at[1, f], left,
        ))
    RA[me] = CA[me]
    for i in others:
        landed(RA.at[i], ar_sem.at[i], member(i))
    total = RA[0]
    for i in range(1, members):
        total = total + RA[i]
    turned = pltpu.roll(total, 64, 1)
    left_half = lane16 < 64
    r_part = jnp.where(left_half, total[0:16], turned[16:32])
    d_part = jnp.where(left_half, turned[0:16], total[16:32])
    QB[z] = substeps(r_part, d_part)[-1][0]
    DB[z] = d_part
    for i in spots:
        sent.append(send(QB.at[z], QB.at[z], qs_sem.at[i], qr_sem.at[z], ring(i)))
    for i in spots:
        sent.append(send(DB.at[z], DB.at[z], ds_sem.at[i], dr_sem.at[z], ring(i)))

    def outside(ref, *at):
        hollow = jnp.zeros((HALO, rows, LANES), F32)

        @pl.when(g == 0)
        def _():
            ref[(*at, pl.ds(0, HALO), body_rows)] = hollow

        @pl.when(g == tiles - 1)
        def _():
            ref[(*at, pl.ds(HALO + cols, HALO), body_rows)] = hollow

    def diffuse(f):
        landed(U.at[f, pl.ds(0, HALO), body_rows], hr_sem.at[0, f], left)
        landed(U.at[f, pl.ds(HALO + cols, HALO), body_rows], hr_sem.at[1, f], right)
        outside(U, f)
        for s in range(ITERS):
            src = U.at[f] if s == 0 else W.at[(s - 1) % 2]
            lo, n = s + 1, wide - 2 * (s + 1)
            lane = iota((n, 8, LANES), 2)
            acc = jnp.zeros((8, LANES), F32)
            for k in range(blocks):
                r = PAD + 8 * k
                cur = src[lo : lo + n, r : r + 8]
                below = src[lo : lo + n, r - 4 : r + 4]
                above = src[lo : lo + n, r + 4 : r + 12]
                south = pltpu.roll(jnp.where(lane == LANES - 1, below, cur), 1, 2)
                north_of = pltpu.roll(jnp.where(lane == 0, above, cur), LANES - 1, 2)
                around = (src[lo - 1 : lo - 1 + n, r : r + 8] + src[lo + 1 : lo + 1 + n, r : r + 8]) + (
                    south + north_of
                )
                new = (1.0 - 4.0 * DIFFUSION) * cur + DIFFUSION * around
                mine = new[HALO - lo : HALO - lo + cols]
                if s + 1 < ITERS:
                    W[s % 2, lo : lo + n, r : r + 8] = new
                else:
                    O[f, :, 8 * k : 8 * k + 8] = mine
                gap = D[f, :, 8 * k : 8 * k + 8] - mine
                acc = acc + jnp.sum(gap * gap, axis=0)
            if s + 1 < ITERS:
                outside(W, s % 2)
            ACC[s * fields + f] = acc

    early = fields - 1
    lax.fori_loop(0, early, lambda f, c: (diffuse(f), c)[1], 0)

    for i in spots:
        landed(QB.at[i], qr_sem.at[i], ring(i))
    q_sum = QB[0]
    for i in range(1, RING):
        q_sum = q_sum + QB[i]
    QC[me] = q_sum
    for i in others:
        sent.append(send(QC.at[me], QC.at[me], cs_sem.at[i], cr_sem.at[me], member(i)))

    lax.fori_loop(early, fields, lambda f, c: (diffuse(f), c)[1], 0)
    local = jnp.zeros((16, LANES), F32)
    for i in range(ITERS * fields):
        local = jnp.where(row16 == i, jnp.sum(ACC[i], axis=0, keepdims=True), local)
    SB[z] = local
    for i in spots:
        sent.append(send(SB.at[z], SB.at[z], ss_sem.at[i], sr_sem.at[z], ring(i)))

    for i in spots:
        landed(DB.at[i], dr_sem.at[i], ring(i))
    d_sum = DB[0]
    for i in range(1, RING):
        d_sum = d_sum + DB[i]
    ones, none = jnp.ones_like(d_sum), jnp.zeros_like(d_sum)
    from_r = substeps(ones, none)[-1][0]
    from_d = substeps(none, d_sum)[-1][0]
    r_sum = (q_sum - from_d) / from_r
    energy = jnp.zeros((16, LANES), F32)
    weight = -0.25 * (east + 1.0) * (north + 1.0)
    mine16 = jnp.where(upper, f_low + 1, f_low)
    for s, (t, r, v) in enumerate(substeps(r_sum, d_sum)):
        part = jnp.sum(weight * t * (r + v), axis=0, keepdims=True)
        energy = jnp.where(row16 == s * fields + mine16, part, energy)

    for i in others:
        landed(QC.at[i], cr_sem.at[i], member(i))
    for h in range(fields // 2):
        parts = []
        for l in range(levels):
            packed = QC[h * levels + l]
            parts += [packed, pltpu.roll(packed, 64, 1)]
        modal = jnp.dot(
            to_grid, jnp.concatenate(parts, axis=0), precision=HIGHEST, preferred_element_type=F32
        )
        for k in range(2):
            mine = jnp.where(lane_g // 32 == k, modal, 0.0)
            mine = mine + pltpu.roll(mine, 32, 1)
            mine = mine + pltpu.roll(mine, 64, 1)
            high = mine.astype(jnp.bfloat16).astype(F32)
            mine = jnp.where(lane_g < 64, high, mine - high)
            PS[2 * h + k] = jnp.concatenate(
                [jnp.where(odd_chunk, 0.0, mine), jnp.where(odd_chunk, mine, 0.0)], axis=1
            ).astype(jnp.bfloat16)
    for k in range(0, blocks, 2):
        quad = [T[:, pl.ds((2 * k + i) * LANES, LANES)] for i in range(4)]
        table = jnp.concatenate(
            [jnp.concatenate(quad[0::2], axis=1), jnp.concatenate(quad[1::2], axis=1)], axis=0
        )
        for f in range(fields):
            tend = jnp.dot(PS[f], table, preferred_element_type=F32)
            for i in range(2):
                at = pl.ds(8 * (k + i), 8)
                O[f, :, at] = O[f, :, at] + tend[:, i * LANES : (i + 1) * LANES].reshape(cols, 8, LANES)
        for t in range(2 * k, 2 * k + 4):
            pltpu.make_async_copy(
                o_view.at[:, :, t], o_hbm.at[:, :, :, pl.ds(t * LANES, LANES)], out_sem
            ).start()

    for i in spots:
        landed(SB.at[i], sr_sem.at[i], ring(i))
    sums = SB[0]
    for i in range(1, RING):
        sums = sums + SB[i]
    EB[me] = sums + energy
    for i in others:
        sent.append(send(EB.at[me], EB.at[me], es_sem.at[i], er_sem.at[me], member(i)))
    for i in others:
        landed(EB.at[i], er_sem.at[i], member(i))
    sums = EB[0]
    for i in range(1, members):
        sums = sums + EB[i]
    cells = float(levels * east * north)
    value = jnp.sqrt(jnp.maximum(jnp.sum(sums, axis=1, keepdims=True) / cells, 0.0))
    spread = jnp.where(row16 % fields == lane16, value, 0.0)
    row8 = iota((8, LANES), 0)
    log = jnp.zeros((8, LANES), F32)
    for s in range(ITERS):
        line = jnp.sum(spread[s * fields : (s + 1) * fields], axis=0, keepdims=True)
        log = jnp.where(row8 == s, line, log)
    res_ref[...] = log[:ITERS, :fields]

    for copy in sent:
        copy.wait_send()
    pltpu.make_async_copy(O, O, out_sem).wait()


def solution(mesh):
    tiles = mesh.shape["gx"]
    members = tiles // RING

    def local(model_state, driving, mode_east, mode_north, level_class, nudge_table):
        fields, levels, cols, north = model_state.shape
        rows = levels * north // LANES
        wide, high_rows = cols + 2 * HALO, rows + 2 * PAD
        vm = lambda *shape: pltpu.VMEM(shape, F32)
        dma = lambda *shape: pltpu.SemaphoreType.DMA(shape)
        smem = pl.BlockSpec(memory_space=pltpu.SMEM)
        anyw = pl.BlockSpec(memory_space=pl.ANY)
        scratch = [
            vm(fields, wide, high_rows, LANES), vm(fields, cols, rows, LANES), vm(fields, cols, rows, LANES),
            vm(2, wide, high_rows, LANES), pltpu.VMEM((LANES, north), jnp.bfloat16),
            vm(members, 32, LANES), vm(members, 32, LANES),
            vm(RING, 16, LANES), vm(RING, 16, LANES), vm(members, 16, LANES),
            vm(RING, 16, LANES), vm(members, 16, LANES),
            vm(ITERS * fields, 8, LANES), pltpu.VMEM((fields, 8 * cols, 2 * LANES), jnp.bfloat16),
            dma(2, fields), pltpu.SemaphoreType.DMA, dma(2, fields), dma(2, fields),
            dma(members), dma(members), dma(RING), dma(RING), dma(RING), dma(RING),
            dma(members), dma(members), dma(RING), dma(RING), dma(members), dma(members),
        ]
        turn = (0, 2, 1, 3)
        nudged, log = pl.pallas_call(
            functools.partial(kernel, tiles),
            out_shape=(
                jax.ShapeDtypeStruct((fields, cols, levels, north), F32),
                jax.ShapeDtypeStruct((ITERS, fields), F32),
            ),
            in_specs=[anyw, anyw, smem, smem, smem, smem],
            out_specs=(anyw, pl.BlockSpec(memory_space=pltpu.VMEM)),
            scratch_shapes=scratch,
            compiler_params=pltpu.CompilerParams(collective_id=0, has_side_effects=True),
        )(
            model_state.transpose(turn), driving.transpose(turn),
            mode_east, mode_north, level_class, nudge_table,
        )
        return nudged.transpose(turn), log

    tile = P("ens", None, "gx", None)
    return jax.shard_map(
        local, mesh=mesh, in_specs=(tile, tile, P(), P(), P(), P()),
        out_specs=(tile, P("ens", None)), check_vma=False,
    )
```

```python
import functools

import jax
import jax.numpy as jnp
import numpy as np
from jax import lax
from jax.experimental import pallas as pl
from jax.experimental.pallas import tpu as pltpu
from jax.sharding import PartitionSpec as P

ITERS = 4
DIFFUSION = 0.24
CORES = 2
RING = 16
MESH = pl.DeviceIdType.MESH
HIGHEST = lax.Precision.HIGHEST
F32 = jnp.float32
LANES = 128
HALO = 4
PAD = 8
STRIPS = 4


def iota(shape, dim):
    return lax.broadcasted_iota(jnp.int32, shape, dim)


def pick(ref, which, count):
    out = jnp.zeros(which.shape, F32)
    for i in range(count):
        out = jnp.where(which == i, ref[i].astype(F32), out)
    return out


def sine(product, period):
    turns = jnp.floor(product * (1.0 / period) + 0.5)
    x = (product - turns * period) * (np.pi / period)
    odd = turns - 2.0 * jnp.floor(turns * 0.5)
    y = x * x
    poly = 1.0 / 6227020800.0
    for c in (-1.0 / 39916800.0, 1.0 / 362880.0, -1.0 / 5040.0, 1.0 / 120.0, -1.0 / 6.0, 1.0):
        poly = poly * y + c
    return x * poly * (1.0 - 2.0 * odd)


def split(value):
    high = value.astype(jnp.bfloat16)
    return high, (value - high.astype(F32)).astype(jnp.bfloat16)


def kernel(
    tiles, u_hbm, d_hbm, me_hbm, mn_hbm, lc_hbm, nt_hbm, O, log_ref,
    me_ref, mn_ref, lc_ref, nt_ref, U, D, W, T, CA, RA, QB, XP, XB, QC, SB, EB, ACC, PS,
    small_sem, in_sem, edge_sem, sems,
):
    fields, cols, levels, north = u_hbm.shape
    kx, ky = me_ref.shape[0], mn_ref.shape[0]
    east = cols * tiles
    members = tiles // RING
    chunks = north // LANES
    blocks = chunks // 2
    wide = cols + 2 * HALO
    rows = 8 * blocks
    high_rows = rows + 2 * PAD
    own = pl.ds(HALO, cols)
    g = lax.axis_index("gx")
    core = lax.rem(g, CORES)
    z = lax.rem(g // CORES, RING)
    xi = g // (CORES * RING)
    me = xi * CORES + core

    def member(i):
        return {"gx": ((i // CORES) * RING + z) * CORES + lax.rem(i, CORES)}

    def ring(i):
        return {"gx": (xi * RING + i) * CORES + core}

    right = {"gx": lax.rem(g + 1, tiles)}
    left = {"gx": lax.rem(g + tiles - 1, tiles)}
    others = [lax.rem(me + k, members) for k in range(1, members)]
    far_first = sorted(range(1, RING), key=lambda k: -min(k, RING - k))
    spots = [lax.rem(z + k, RING) for k in far_first]

    u_view = U.reshape(fields, wide, high_rows // levels, levels, LANES)
    d_view = D.reshape(fields, cols, chunks, levels, LANES)
    skip = PAD // levels
    small = []
    for i, (hbm, ref) in enumerate(((me_hbm, me_ref), (mn_hbm, mn_ref), (lc_hbm, lc_ref), (nt_hbm, nt_ref))):
        small.append(pltpu.make_async_copy(hbm, ref, small_sem.at[i]))
        small[-1].start()
    for h in range(0, fields, 2):
        two = pl.ds(h, 2)
        for i in range(2):
            for t in range(chunks):
                hbm, dst = (
                    (u_hbm, u_view.at[two, own, skip + t]) if i == 0 else (d_hbm, d_view.at[two, :, t])
                )
                pltpu.make_async_copy(
                    hbm.at[two, :, :, pl.ds(t * LANES, LANES)], dst, in_sem.at[i, h // 2]
                ).start()

    def loaded(i, h):
        two = pl.ds(h, 2)
        ref = U.at[two, own, pl.ds(PAD, rows)] if i == 0 else D.at[two]
        pltpu.make_async_copy(ref, ref, in_sem.at[i, h // 2]).wait()

    barrier = pltpu.get_barrier_semaphore()
    greeted = [member(i) for i in others] + [ring(i) for i in spots] + [left, right]
    for who in greeted:
        pl.semaphore_signal(barrier, inc=1, device_id=who, device_id_type=MESH)

    for copy in small:
        copy.wait()
    row32 = iota((32, LANES), 0)
    lane32 = iota((32, LANES), 1)
    modes_n = pick(mn_ref, row32, ky)
    for c in range(chunks):
        place = (lane32 + (c * LANES + 1)).astype(F32)
        high, low = split(sine(modes_n * place, float(north + 1)))
        at = pl.ds(c * LANES, LANES)
        both = jnp.concatenate([high, low], axis=0)
        T[0:64, at] = both
        T[64:128, at] = both
    first = g * cols
    count = 8 * cols
    grid_rows = 8 * ((count + LANES - 1) // LANES) * (LANES // 8)
    row_m, lane_m = iota((LANES, grid_rows), 0), iota((LANES, grid_rows), 1)
    mode_m = pick(me_ref, iota((LANES, LANES), 0) % 32, kx)
    mode_m = jnp.concatenate([mode_m] * (grid_rows // LANES), axis=1)
    to_modes = jnp.where(
        (lane_m < count) & (row_m // 32 == lane_m % 4),
        sine(mode_m * (lane_m // 8 + first + 1).astype(F32), float(east + 1)), 0.0,
    )
    row_g, lane_g = iota((count, LANES), 0), iota((count, LANES), 1)
    mode_g = jnp.concatenate([pick(me_ref, iota((8, LANES), 1) % 32, kx)] * cols, axis=0)
    to_grid = jnp.where(
        row_g % 4 == lane_g // 32,
        sine(mode_g * (row_g // 8 + first + 1).astype(F32), float(east + 1)), 0.0,
    )
    edge = jnp.zeros((wide, PAD, LANES), F32)
    for f in range(fields):
        U[f, :, 0:PAD] = edge
        U[f, :, PAD + rows : high_rows] = edge
    for s in range(2):
        W[s, :, 0:PAD] = edge
        W[s, :, PAD + rows : high_rows] = edge

    row16 = iota((16, LANES), 0)
    lane16 = iota((16, LANES), 1)
    f_low = 2 * (me // levels)
    my_class = lc_ref[lax.rem(me, levels)]
    w_low, w_up = nt_ref[f_low, my_class], nt_ref[f_low + 1, my_class]
    share = 16 // RING

    def constants(top, count):
        lane = iota((count, LANES), 1)
        a = iota((count, LANES), 0) + top + jnp.where(lane >= 64, 16, 0)
        half_e = sine(pick(me_ref, a, kx), 2.0 * (east + 1))
        half_n = sine(pick(mn_ref, lane % 32, ky), 2.0 * (north + 1))
        fade = (4.0 * DIFFUSION) * (half_e * half_e + half_n * half_n)
        return fade, jnp.where(lane % 64 >= 32, w_up, w_low)

    def substeps(fade, w, r, d):
        lam = 1.0 - fade
        t = jnp.zeros_like(r)
        v = r
        out = []
        for _ in range(ITERS):
            t = lam * t + w * r
            r = (lam - w) * r + fade * d
            v = lam * v + fade * d
            out.append((t, r, v))
        return out

    all_modes = constants(0, 16)
    my_modes = constants(z * share, share)

    norm = 4.0 / ((east + 1) * (north + 1))
    odd_chunk = row_g % 8 >= 4
    contract_lanes = (((1,), (1,)), ((), ()))
    for h in range(0, fields, 2):
        loaded(0, h)
        loaded(1, h)
        acc_r = acc_d = None
        held = []
        for k in range(blocks):
            at = pl.ds(8 * k, 8)
            d = D[h : h + 2, :, at]
            r = d - U[h : h + 2, own, pl.ds(PAD + 8 * k, 8)]
            high, low = split(r.reshape(2 * count, LANES))
            table = jnp.concatenate(
                [T[0:64, pl.ds((2 * k + p) * LANES, LANES)] for p in range(2)], axis=0
            )
            out = lax.dot_general(
                jnp.concatenate([high, low], axis=1), jnp.concatenate([table, table], axis=1),
                contract_lanes, preferred_element_type=F32,
            )
            acc_r = out if acc_r is None else acc_r + out
            held.append((d.reshape(2 * count, LANES).astype(jnp.bfloat16), table))
            if len(held) == 2:
                out = lax.dot_general(
                    jnp.concatenate([held[0][0], held[1][0]], axis=1),
                    jnp.concatenate([held[0][1], held[1][1]], axis=1),
                    contract_lanes, preferred_element_type=F32,
                )
                acc_d = out if acc_d is None else acc_d + out
                held = []
        mix = jnp.zeros((count, LANES), F32)
        for i, acc in enumerate((acc_r, acc_d)):
            acc = acc + pltpu.roll(acc, 32, 1)
            for j in range(2):
                mine = acc[j * count : (j + 1) * count]
                slot = 2 * i + j
                even, odd = ((slot - 1) % 4) * 32, ((slot + 1) % 4) * 32
                even = pltpu.roll(mine, even, 1) if even else mine
                odd = pltpu.roll(mine, odd, 1) if odd else mine
                mix = jnp.where(lane_g // 32 == slot, jnp.where(odd_chunk, odd, even), mix)
        if grid_rows > count:
            mix = jnp.concatenate([mix, jnp.zeros((grid_rows - count, LANES), F32)], axis=0)
        modal = norm * jnp.dot(to_modes, mix, precision=HIGHEST, preferred_element_type=F32)
        for l in range(levels):
            CA[(h // 2) * levels + l] = modal[32 * l : 32 * l + 32]

    pl.semaphore_wait(barrier, len(greeted))

    def send(src, dst, phase, who, recv_sem=None):
        pltpu.make_async_remote_copy(
            src_ref=src, dst_ref=dst, send_sem=sems.at[0, phase],
            recv_sem=sems.at[1, phase] if recv_sem is None else recv_sem,
            device_id=who, device_id_type=MESH,
        ).start()

    def both_ends(ref, phase, recv_sem=None):
        return pltpu.make_async_remote_copy(
            src_ref=ref, dst_ref=ref, send_sem=sems.at[0, phase],
            recv_sem=sems.at[1, phase] if recv_sem is None else recv_sem,
            device_id=right, device_id_type=MESH,
        )

    EDGE, SLICE, SHARE, SUM, BACK, PART, LOG = range(7)
    body_rows = pl.ds(PAD, rows)
    west, inner_west = pl.ds(0, HALO), pl.ds(HALO, HALO)
    inner_east, east_edge = pl.ds(cols, HALO), pl.ds(HALO + cols, HALO)

    def send_edges(f):
        send(U.at[f, inner_east, body_rows], U.at[f, west, body_rows], EDGE, right, edge_sem.at[0, f])
        send(U.at[f, inner_west, body_rows], U.at[f, east_edge, body_rows], EDGE, left, edge_sem.at[1, f])

    send_edges(0)
    for i in others:
        send(CA.at[i], RA.at[me], SLICE, member(i))
    for f in range(1, fields):
        send_edges(f)
    RA[me] = CA[me]

    def outside(ref, *at):
        hollow = jnp.zeros((HALO, rows, LANES), F32)

        @pl.when(g == 0)
        def _():
            ref[(*at, pl.ds(0, HALO), body_rows)] = hollow

        @pl.when(g == tiles - 1)
        def _():
            ref[(*at, pl.ds(HALO + cols, HALO), body_rows)] = hollow

    def diffuse(f):
        both_ends(U.at[f, west, body_rows], EDGE, edge_sem.at[0, f]).wait_recv()
        both_ends(U.at[f, east_edge, body_rows], EDGE, edge_sem.at[1, f]).wait_recv()
        outside(U, f)
        for s in range(ITERS):
            src = U.at[f] if s == 0 else W.at[(s - 1) % 2]
            lo, hi = s + 1, wide - (s + 1)
            cuts = [lo + (hi - lo) * i // STRIPS for i in range(STRIPS + 1)]
            acc = jnp.zeros((8, LANES), F32)
            for k in range(blocks):
                r = PAD + 8 * k
                for x0, x1 in zip(cuts[:-1], cuts[1:]):
                    near = src[x0 - 1 : x1 + 1, r : r + 8]
                    cur = near[1:-1]
                    lane = iota((x1 - x0, 8, LANES), 2)
                    below = src[x0:x1, r - 4 : r + 4]
                    above = src[x0:x1, r + 4 : r + 12]
                    south = pltpu.roll(jnp.where(lane == LANES - 1, below, cur), 1, 2)
                    north_of = pltpu.roll(jnp.where(lane == 0, above, cur), LANES - 1, 2)
                    around = (near[:-2] + near[2:]) + (south + north_of)
                    new = (1.0 - 4.0 * DIFFUSION) * cur + DIFFUSION * around
                    if s + 1 < ITERS:
                        W[s % 2, x0:x1, r : r + 8] = new
                    y0, y1 = max(x0, HALO), min(x1, HALO + cols)
                    if y0 >= y1:
                        continue
                    at = slice(y0 - HALO, y1 - HALO)
                    new = new[y0 - x0 : y1 - x0]
                    if s + 1 == ITERS:
                        O[f, at, 8 * k : 8 * k + 8] = new
                    gap = D[f, at, 8 * k : 8 * k + 8] - new
                    acc = acc + jnp.sum(gap * gap, axis=0)
            if s + 1 < ITERS:
                outside(W, s % 2)
            ACC[s * fields + f] = acc

    diffuse(0)
    both_ends(RA.at[pl.ds(0, members - 1)], SLICE).wait_recv()
    total = RA[0]
    for i in range(1, members):
        total = total + RA[i]
    turned = pltpu.roll(total, 64, 1)
    left_half = lane16 < 64
    r_part = jnp.where(left_half, total[0:16], turned[16:32])
    d_part = jnp.where(left_half, turned[0:16], total[16:32])
    for i in range(RING):
        part = slice(i * share, (i + 1) * share)
        XP[i] = jnp.concatenate([r_part[part], d_part[part]], axis=0)
    for i in spots:
        send(XP.at[i], XB.at[z], SHARE, ring(i))
    QB[z] = substeps(*all_modes, r_part, d_part)[-1][0]
    for i in spots:
        send(QB.at[z], QB.at[z], SUM, ring(i))
    XB[z] = XP[z]
    lax.fori_loop(1, fields, lambda f, c: (diffuse(f), c)[1], 0)

    both_ends(XB.at[pl.ds(0, RING - 1)], SHARE).wait_recv()
    shares = XB[0]
    for i in range(1, RING):
        shares = shares + XB[i]
    r_sum, d_sum = shares[:share], shares[share:]
    energy = jnp.zeros((16, LANES), F32)
    weight = -0.25 * (east + 1.0) * (north + 1.0)
    my_field = jnp.where(lane16 % 64 >= 32, f_low + 1, f_low)
    for s, (t, r, v) in enumerate(substeps(*my_modes, r_sum, d_sum)):
        part = jnp.sum(weight * t * (r + v), axis=0, keepdims=True)
        energy = jnp.where(row16 == s * fields + my_field, part, energy)
    for i in range(ITERS * fields):
        energy = energy + jnp.where(row16 == i, jnp.sum(ACC[i], axis=0, keepdims=True), 0.0)
    energy = jnp.sum(energy, axis=1, keepdims=True)
    SB[z] = jnp.sum(jnp.where(row16 == lane16, energy, 0.0), axis=0, keepdims=True)
    for i in spots:
        send(SB.at[z], SB.at[z], PART, ring(i))

    both_ends(QB.at[pl.ds(0, RING - 1)], SUM).wait_recv()
    q_sum = QB[0]
    for i in range(1, RING):
        q_sum = q_sum + QB[i]
    QC[me] = q_sum
    for i in others:
        send(QC.at[me], QC.at[me], BACK, member(i))

    both_ends(QC.at[pl.ds(0, members - 1)], BACK).wait_recv()
    for h in range(fields // 2):
        parts = []
        for l in range(levels):
            packed = QC[h * levels + l]
            parts += [packed, pltpu.roll(packed, 64, 1)]
        modal = jnp.dot(
            to_grid, jnp.concatenate(parts, axis=0), precision=HIGHEST, preferred_element_type=F32
        )
        for k in range(2):
            mine = jnp.where(lane_g // 32 == k, modal, 0.0)
            mine = mine + pltpu.roll(mine, 32, 1)
            mine = mine + pltpu.roll(mine, 64, 1)
            high = mine.astype(jnp.bfloat16).astype(F32)
            mine = jnp.where(lane_g < 64, high, mine - high)
            PS[2 * h + k] = jnp.concatenate(
                [jnp.where(odd_chunk, 0.0, mine), jnp.where(odd_chunk, mine, 0.0)], axis=1
            ).astype(jnp.bfloat16)
    for k in range(0, blocks, 2):
        quad = [T[:, pl.ds((2 * k + i) * LANES, LANES)] for i in range(4)]
        table = jnp.concatenate(
            [jnp.concatenate(quad[0::2], axis=1), jnp.concatenate(quad[1::2], axis=1)], axis=0
        )
        for f in range(fields):
            tend = jnp.dot(PS[f], table, preferred_element_type=F32)
            for i in range(2):
                at = pl.ds(8 * (k + i), 8)
                O[f, :, at] = O[f, :, at] + tend[:, i * LANES : (i + 1) * LANES].reshape(cols, 8, LANES)

    both_ends(SB.at[pl.ds(0, RING - 1)], PART).wait_recv()
    sums = SB[0]
    for i in range(1, RING):
        sums = sums + SB[i]
    EB[me] = sums
    for i in others:
        send(EB.at[me], EB.at[me], LOG, member(i))
    both_ends(EB.at[pl.ds(0, members - 1)], LOG).wait_recv()
    sums = EB[0]
    for i in range(1, members):
        sums = sums + EB[i]
    cells = float(levels * east * north)
    value = jnp.broadcast_to(jnp.sqrt(jnp.maximum(sums / cells, 0.0)), (8, LANES))
    row8 = iota((8, LANES), 0)
    log = value
    for s in range(1, ITERS):
        log = jnp.where(row8 == s, pltpu.roll(value, LANES - s * fields, 1), log)
    log_ref[...] = log

    both_ends(U.at[:, pl.ds(0, 2 * HALO), body_rows], EDGE).wait_send()
    for phase, buf in ((SLICE, RA), (SHARE, XB), (SUM, QB), (BACK, QC), (PART, SB), (LOG, EB)):
        both_ends(buf.at[pl.ds(0, buf.shape[0] - 1)], phase).wait_send()


def writer(O, log_ref, o_hbm, res_ref, sem):
    fields, cols, levels, north = o_hbm.shape
    chunks = north // LANES
    o_view = O.reshape(fields, cols, chunks, levels, LANES)
    for t in range(chunks):
        pltpu.make_async_copy(
            o_view.at[:, :, t], o_hbm.at[:, :, :, pl.ds(t * LANES, LANES)], sem
        ).start()
    res_ref[...] = log_ref[: res_ref.shape[0], : res_ref.shape[1]]
    pltpu.make_async_copy(O, O, sem).wait()


def solution(mesh):
    tiles = mesh.shape["gx"]
    members = tiles // RING

    def local(model_state, driving, mode_east, mode_north, level_class, nudge_table):
        fields, levels, cols, north = model_state.shape
        rows = levels * north // LANES
        wide, high_rows = cols + 2 * HALO, rows + 2 * PAD
        share = 16 // RING
        vm = lambda *shape: pltpu.VMEM(shape, F32)
        dma = lambda *shape: pltpu.SemaphoreType.DMA(shape)
        hbm = pl.BlockSpec(memory_space=pltpu.HBM)
        smem = lambda ref: pltpu.SMEM(ref.shape, ref.dtype)
        table = nudge_table.T
        scratch = [
            smem(mode_east), smem(mode_north), smem(level_class), smem(table),
            vm(fields, wide, high_rows, LANES), vm(fields, cols, rows, LANES),
            vm(2, wide, high_rows, LANES), pltpu.VMEM((LANES, north), jnp.bfloat16),
            vm(members, 32, LANES), vm(members, 32, LANES),
            vm(RING, 16, LANES), vm(RING, 2 * share, LANES), vm(RING, 2 * share, LANES), vm(members, 16, LANES),
            vm(RING, 1, LANES), vm(members, 1, LANES),
            vm(ITERS * fields, 8, LANES), pltpu.VMEM((fields, 8 * cols, 2 * LANES), jnp.bfloat16),
            dma(4), dma(2, fields // 2), dma(2, fields), dma(2, 7),
        ]
        turn = (0, 2, 1, 3)
        inner = pl.BlockSpec(memory_space=pltpu.VMEM)
        grid, log = pl.pallas_call(
            functools.partial(kernel, tiles),
            out_shape=(
                vm(fields, cols, rows, LANES),
                vm(8, LANES),
            ),
            in_specs=[hbm] * 6,
            out_specs=(inner, inner),
            scratch_shapes=scratch,
            compiler_params=pltpu.CompilerParams(
                collective_id=0, has_side_effects=True, vmem_limit_bytes=60 * 2**20
            ),
        )(
            model_state.transpose(turn), driving.transpose(turn),
            mode_east, mode_north, level_class, table,
        )
        nudged, log = pl.pallas_call(
            writer,
            out_shape=(
                jax.ShapeDtypeStruct((fields, cols, levels, north), F32),
                jax.ShapeDtypeStruct((ITERS, fields), F32),
            ),
            in_specs=[inner, inner],
            out_specs=(hbm, inner),
            scratch_shapes=[pltpu.SemaphoreType.DMA],
            compiler_params=pltpu.CompilerParams(vmem_limit_bytes=8 * 2**20),
        )(grid, log)
        return nudged.transpose(turn), log

    tile = P("ens", None, "gx", None)
    return jax.shard_map(
        local, mesh=mesh, in_specs=(tile, tile, P(), P(), P(), P()),
        out_specs=(tile, P("ens", None)), check_vma=False,
    )
```

```python
import functools

import jax
import jax.numpy as jnp
import numpy as np
from jax import lax
from jax.experimental import pallas as pl
from jax.experimental.pallas import tpu as pltpu
from jax.sharding import PartitionSpec as P

ITERS = 4
DIFFUSION = 0.24
CORES = 2
RING = 16
MESH = pl.DeviceIdType.MESH
HIGHEST = lax.Precision.HIGHEST
F32 = jnp.float32
LANES = 128
HALO = 4
PAD = 8
INNER_STRIPS = 3
AHEAD = 1


def iota(shape, dim):
    return lax.broadcasted_iota(jnp.int32, shape, dim)


def pick(ref, which, count):
    out = jnp.zeros(which.shape, F32)
    for i in range(count):
        out = jnp.where(which == i, ref[i].astype(F32), out)
    return out


def sine(product, period):
    turns = jnp.floor(product * (1.0 / period) + 0.5)
    x = (product - turns * period) * (np.pi / period)
    odd = turns - 2.0 * jnp.floor(turns * 0.5)
    y = x * x
    poly = 1.0 / 6227020800.0
    for c in (-1.0 / 39916800.0, 1.0 / 362880.0, -1.0 / 5040.0, 1.0 / 120.0, -1.0 / 6.0, 1.0):
        poly = poly * y + c
    return x * poly * (1.0 - 2.0 * odd)


def split(value):
    high = value.astype(jnp.bfloat16)
    return high, (value - high.astype(F32)).astype(jnp.bfloat16)


def kernel(
    tiles, u_hbm, d_hbm, me_hbm, mn_hbm, lc_hbm, nt_hbm, O, log_ref,
    me_ref, mn_ref, lc_ref, nt_ref, U, D, W, T, XD, PX, XS, XB, Y, YP, QD, ACC, PS,
    small_sem, in_sem, edge_sem, sems, heard,
):
    fields, cols, levels, north = u_hbm.shape
    kx, ky = me_ref.shape[0], mn_ref.shape[0]
    east = cols * tiles
    chips = tiles // CORES
    share = 16 * levels // chips
    chunks = north // LANES
    blocks = chunks // 2
    wide = cols + 2 * HALO
    rows = 8 * blocks
    high_rows = rows + 2 * PAD
    own = pl.ds(HALO, cols)
    g = lax.axis_index("gx")
    core = lax.rem(g, CORES)
    z = lax.rem(g // CORES, RING)
    xi = g // (CORES * RING)
    chip = g // CORES
    partner = {"gx": chip * CORES + (CORES - 1 - core)}
    right = {"gx": lax.rem(g + 1, tiles)}
    left = {"gx": lax.rem(g + tiles - 1, tiles)}
    across = chips // RING
    far_first = sorted(range(RING), key=lambda k: -min(k, RING - k))
    z_spots = [lax.rem(z + k, RING) for k in far_first]
    x_spots = [lax.rem(xi + k, across) * RING for k in range(across)]
    others = [x_spots[i] + z_spots[k] for k in range(RING) for i in range(across)]
    del others[RING * across - across]

    def peer(i):
        return {"gx": i * CORES + core}

    barrier = pltpu.get_barrier_semaphore()
    beside = [lax.rem(z + 1, RING), lax.rem(z + RING - 1, RING)]
    greeted = [partner, left, right] + [peer(x_spots[i] + z) for i in range(1, across)]
    greeted += [peer(x + there) for there in beside for x in x_spots]
    for who in greeted:
        pl.semaphore_signal(barrier, inc=1, device_id=who, device_id_type=MESH)
    rounds = [1 << i for i in range(8) if 4 << i <= RING]

    def hear(i):
        if i < len(rounds):
            pl.semaphore_wait(heard.at[i], 2)

    def tell(i):
        if i < len(rounds):
            for there in (lax.rem(z + rounds[i], RING), lax.rem(z + RING - rounds[i], RING)):
                pl.semaphore_signal(
                    heard.at[i], inc=1, device_id=peer(xi * RING + there), device_id_type=MESH
                )

    u_view = U.reshape(fields, wide, high_rows // levels, levels, LANES)
    d_view = D.reshape(fields, cols, chunks, levels, LANES)
    skip = PAD // levels
    small = []
    for i, (hbm, ref) in enumerate(((me_hbm, me_ref), (mn_hbm, mn_ref), (lc_hbm, lc_ref), (nt_hbm, nt_ref))):
        small.append(pltpu.make_async_copy(hbm, ref, small_sem.at[i]))
        small[-1].start()
    for h in range(0, fields, 2):
        two = pl.ds(h, 2)
        for i in range(2):
            for t in range(chunks):
                hbm, dst = (
                    (u_hbm, u_view.at[two, own, skip + t]) if i == 0 else (d_hbm, d_view.at[two, :, t])
                )
                pltpu.make_async_copy(
                    hbm.at[two, :, :, pl.ds(t * LANES, LANES)], dst, in_sem.at[i, h // 2]
                ).start()

    def loaded(i, h):
        two = pl.ds(h, 2)
        ref = U.at[two, own, pl.ds(PAD, rows)] if i == 0 else D.at[two]
        pltpu.make_async_copy(ref, ref, in_sem.at[i, h // 2]).wait()

    for copy in small:
        copy.wait()
    row32 = iota((32, LANES), 0)
    lane32 = iota((32, LANES), 1)
    modes_n = pick(mn_ref, row32, ky)
    for c in range(chunks):
        place = (lane32 + (c * LANES + 1)).astype(F32)
        high, low = split(sine(modes_n * place, float(north + 1)))
        at = pl.ds(c * LANES, LANES)
        both = jnp.concatenate([high, low], axis=0)
        T[0:64, at] = both
        T[64:128, at] = both
    first = g * cols
    count = 8 * cols
    grid_rows = 8 * ((count + LANES - 1) // LANES) * (LANES // 8)
    row_m, lane_m = iota((LANES, grid_rows), 0), iota((LANES, grid_rows), 1)
    mode_m = pick(me_ref, iota((LANES, LANES), 0) % 32, kx)
    mode_m = jnp.concatenate([mode_m] * (grid_rows // LANES), axis=1)
    to_modes = jnp.where(
        (lane_m < count) & (row_m // 32 == lane_m % 4),
        sine(mode_m * (lane_m // 8 + first + 1).astype(F32), float(east + 1)), 0.0,
    )
    row_g, lane_g = iota((count, LANES), 0), iota((count, LANES), 1)
    mode_g = jnp.concatenate([pick(me_ref, iota((8, LANES), 1) % 32, kx)] * cols, axis=0)
    to_grid = jnp.where(
        row_g % 4 == lane_g // 32,
        sine(mode_g * (row_g // 8 + first + 1).astype(F32), float(east + 1)), 0.0,
    )
    row16 = iota((16, LANES), 0)
    lane16 = iota((16, LANES), 1)
    f_low = 2 * core
    my_class = lc_ref[(chip * share) // 16]
    w_low, w_up = nt_ref[f_low, my_class], nt_ref[f_low + 1, my_class]

    def constants(top, count):
        lane = iota((count, LANES), 1)
        a = iota((count, LANES), 0) + top + jnp.where(lane >= 64, 16, 0)
        half_e = sine(pick(me_ref, a, kx), 2.0 * (east + 1))
        half_n = sine(pick(mn_ref, lane % 32, ky), 2.0 * (north + 1))
        fade = (4.0 * DIFFUSION) * (half_e * half_e + half_n * half_n)
        return fade, jnp.where(lane % 64 >= 32, w_up, w_low)

    def substeps(fade, w, r, d):
        lam = 1.0 - fade
        t = jnp.zeros_like(r)
        v = r
        out = []
        for _ in range(ITERS):
            t = lam * t + w * r
            r = (lam - w) * r + fade * d
            v = lam * v + fade * d
            out.append((t, r, v))
        return out

    my_modes = constants(lax.rem(chip * share, 16), share)

    pl.semaphore_wait(barrier, len(greeted))
    tell(0)

    def send(src, dst, phase, who, recv_sem=None):
        pltpu.make_async_remote_copy(
            src_ref=src, dst_ref=dst, send_sem=sems.at[0, phase],
            recv_sem=sems.at[1, phase] if recv_sem is None else recv_sem,
            device_id=who, device_id_type=MESH,
        ).start()

    def both_ends(ref, phase, recv_sem=None):
        return pltpu.make_async_remote_copy(
            src_ref=ref, dst_ref=ref, send_sem=sems.at[0, phase],
            recv_sem=sems.at[1, phase] if recv_sem is None else recv_sem,
            device_id=right, device_id_type=MESH,
        )

    EDGE, PAIR, SHARE, ALL, BACK = range(5)
    body_rows = pl.ds(PAD, rows)
    west, inner_west = pl.ds(0, HALO), pl.ds(HALO, HALO)
    inner_east, east_edge = pl.ds(cols, HALO), pl.ds(HALO + cols, HALO)

    def send_edges(f):
        send(U.at[f, inner_east, body_rows], U.at[f, west, body_rows], EDGE, right, edge_sem.at[0, f])
        send(U.at[f, inner_west, body_rows], U.at[f, east_edge, body_rows], EDGE, left, edge_sem.at[1, f])

    norm = 4.0 / ((east + 1) * (north + 1))
    odd_chunk = row_g % 8 >= 4
    contract_lanes = (((1,), (1,)), ((), ()))
    for h in range(0, fields, 2):
        loaded(0, h)
        loaded(1, h)
        acc_r = acc_d = None
        held = []
        for k in range(blocks):
            at = pl.ds(8 * k, 8)
            d = D[h : h + 2, :, at]
            r = d - U[h : h + 2, own, pl.ds(PAD + 8 * k, 8)]
            high, low = split(r.reshape(2 * count, LANES))
            table = jnp.concatenate(
                [T[0:64, pl.ds((2 * k + p) * LANES, LANES)] for p in range(2)], axis=0
            )
            out = lax.dot_general(
                jnp.concatenate([high, low], axis=1), jnp.concatenate([table, table], axis=1),
                contract_lanes, preferred_element_type=F32,
            )
            acc_r = out if acc_r is None else acc_r + out
            held.append((d.reshape(2 * count, LANES).astype(jnp.bfloat16), table))
            if len(held) == 2:
                out = lax.dot_general(
                    jnp.concatenate([held[0][0], held[1][0]], axis=1),
                    jnp.concatenate([held[0][1], held[1][1]], axis=1),
                    contract_lanes, preferred_element_type=F32,
                )
                acc_d = out if acc_d is None else acc_d + out
                held = []
        mix = jnp.zeros((count, LANES), F32)
        for i, acc in enumerate((acc_r, acc_d)):
            acc = acc + pltpu.roll(acc, 32, 1)
            for j in range(2):
                mine = acc[j * count : (j + 1) * count]
                slot = 2 * i + j
                even, odd = ((slot - 1) % 4) * 32, ((slot + 1) % 4) * 32
                even = pltpu.roll(mine, even, 1) if even else mine
                odd = pltpu.roll(mine, odd, 1) if odd else mine
                mix = jnp.where(lane_g // 32 == slot, jnp.where(odd_chunk, odd, even), mix)
        if grid_rows > count:
            mix = jnp.concatenate([mix, jnp.zeros((grid_rows - count, LANES), F32)], axis=0)
        modal = norm * jnp.dot(to_modes, mix, precision=HIGHEST, preferred_element_type=F32)
        turned = pltpu.roll(modal, 64, 1)
        send_edges(h)
        send_edges(h + 1)
        hear(h // 2)
        tell(h // 2 + 1)
        for l in range(levels):
            upper_a, lower_a = slice(32 * l, 32 * l + 16), slice(32 * l + 16, 32 * l + 32)
            XD[h // 2, 32 * l : 32 * l + 16] = jnp.where(lane16 < 64, modal[upper_a], turned[lower_a])
            XD[h // 2, 32 * l + 16 : 32 * l + 32] = jnp.where(lane16 < 64, turned[upper_a], modal[lower_a])

    def outside(ref, *at):
        hollow = jnp.zeros((HALO, rows, LANES), F32)

        @pl.when(g == 0)
        def _():
            ref[(*at, pl.ds(0, HALO), body_rows)] = hollow

        @pl.when(g == tiles - 1)
        def _():
            ref[(*at, pl.ds(HALO + cols, HALO), body_rows)] = hollow

    def update(f, s, bounds, strips):
        src = U.at[f] if s == 0 else W.at[f, s - 1]
        acc = jnp.zeros((8, LANES), F32)
        cuts = []
        for lo, hi in bounds:
            cuts += [(lo + (hi - lo) * i // strips, lo + (hi - lo) * (i + 1) // strips) for i in range(strips)]
        for k in range(blocks):
            r = PAD + 8 * k
            for x0, x1 in cuts:
                near = src[x0 - 1 : x1 + 1, r : r + 8]
                cur = near[1:-1]
                lane = iota((x1 - x0, 8, LANES), 2)
                below = src[x0:x1, r - 4 : r + 4]
                above = src[x0:x1, r + 4 : r + 12]
                south = pltpu.roll(jnp.where(lane == LANES - 1, below, cur), 1, 2)
                north_of = pltpu.roll(jnp.where(lane == 0, above, cur), LANES - 1, 2)
                around = (near[:-2] + near[2:]) + (south + north_of)
                new = (1.0 - 4.0 * DIFFUSION) * cur + DIFFUSION * around
                if s + 1 < ITERS:
                    W[f, s, x0:x1, r : r + 8] = new
                y0, y1 = max(x0, HALO), min(x1, HALO + cols)
                if y0 >= y1:
                    continue
                at = slice(y0 - HALO, y1 - HALO)
                new = new[y0 - x0 : y1 - x0]
                if s + 1 == ITERS:
                    O[f, at, 8 * k : 8 * k + 8] = new
                gap = D[f, at, 8 * k : 8 * k + 8] - new
                acc = acc + jnp.sum(gap * gap, axis=0)
        return acc

    def diffuse_inner(f):
        for s in range(ITERS):
            ACC[s * fields + f] = update(f, s, [(HALO + 1 + s, HALO + cols - 1 - s)], INNER_STRIPS)

    def diffuse_edges(f):
        both_ends(U.at[f, west, body_rows], EDGE, edge_sem.at[0, f]).wait_recv()
        both_ends(U.at[f, east_edge, body_rows], EDGE, edge_sem.at[1, f]).wait_recv()
        outside(U, f)
        for s in range(ITERS):
            spans = [(s + 1, HALO + 1 + s), (HALO + cols - 1 - s, wide - 1 - s)]
            acc = update(f, s, spans, 1)
            ACC[s * fields + f] = ACC[s * fields + f] + acc
            if s + 1 < ITERS:
                outside(W, f, s)

    send(XD.at[CORES - 1 - core], PX, PAIR, partner)
    rim = jnp.zeros((wide, PAD, LANES), F32)
    for f in range(fields):
        for ref in [U.at[f]] + [W.at[f, s] for s in range(ITERS - 1)]:
            ref[:, 0:PAD] = rim
            ref[:, PAD + rows : high_rows] = rim
    lax.fori_loop(0, AHEAD, lambda f, c: (diffuse_inner(f), c)[1], 0)
    both_ends(PX, PAIR).wait_recv()
    total = XD[core] + PX[...]
    for i in range(chips):
        l, top = (i * share) // 16, (i * share) % 16
        XS[i, :share] = total[32 * l + top : 32 * l + top + share]
        XS[i, share:] = total[32 * l + 16 + top : 32 * l + 16 + top + share]
    for i in range(2, len(rounds)):
        hear(i)
        tell(i + 1)
    for i in others:
        send(XS.at[i], XB.at[chip], SHARE, peer(i))
    XB[chip] = XS[chip]
    lax.fori_loop(AHEAD, fields, lambda f, c: (diffuse_inner(f), c)[1], 0)
    lax.fori_loop(0, fields, lambda f, c: (diffuse_edges(f), c)[1], 0)

    both_ends(XB.at[pl.ds(0, chips - 1)], SHARE).wait_recv()
    shares = jnp.sum(XB[...], axis=0)
    r_sum, d_sum = shares[:share], shares[share:]
    energy = jnp.zeros((16, LANES), F32)
    weight = -0.25 * (east + 1.0) * (north + 1.0)
    my_field = jnp.where(lane16 % 64 >= 32, f_low + 1, f_low)
    course = substeps(*my_modes, r_sum, d_sum)
    for s, (t, r, v) in enumerate(course):
        part = jnp.sum(weight * t * (r + v), axis=0, keepdims=True)
        energy = jnp.where(row16 == s * fields + my_field, part, energy)
    for i in range(ITERS * fields):
        energy = energy + jnp.where(row16 == i, jnp.sum(ACC[i], axis=0, keepdims=True), 0.0)
    energy = jnp.sum(energy, axis=1, keepdims=True)
    Y[chip, :share] = course[-1][0]
    Y[chip, share:] = jnp.sum(jnp.where(row16 == lane16, energy, 0.0), axis=0, keepdims=True)
    for i in others:
        send(Y.at[chip], Y.at[chip], ALL, peer(i))
    both_ends(Y.at[pl.ds(0, chips - 1)], ALL).wait_recv()
    send(Y, YP, BACK, partner)
    for i in range(chips):
        QD[core, i * share : (i + 1) * share] = Y[i, :share]

    both_ends(YP, BACK).wait_recv()
    for i in range(chips):
        QD[CORES - 1 - core, i * share : (i + 1) * share] = YP[i, :share]
    for h in range(fields // 2):
        parts = []
        for l in range(levels):
            packed = QD[h, 16 * l : 16 * l + 16]
            parts += [packed, pltpu.roll(packed, 64, 1)]
        modal = jnp.dot(
            to_grid, jnp.concatenate(parts, axis=0), precision=HIGHEST, preferred_element_type=F32
        )
        for k in range(2):
            mine = jnp.where(lane_g // 32 == k, modal, 0.0)
            mine = mine + pltpu.roll(mine, 32, 1)
            mine = mine + pltpu.roll(mine, 64, 1)
            high = mine.astype(jnp.bfloat16).astype(F32)
            mine = jnp.where(lane_g < 64, high, mine - high)
            PS[2 * h + k] = jnp.concatenate(
                [jnp.where(odd_chunk, 0.0, mine), jnp.where(odd_chunk, mine, 0.0)], axis=1
            ).astype(jnp.bfloat16)
    for k in range(0, blocks, 2):
        quad = [T[:, pl.ds((2 * k + i) * LANES, LANES)] for i in range(4)]
        table = jnp.concatenate(
            [jnp.concatenate(quad[0::2], axis=1), jnp.concatenate(quad[1::2], axis=1)], axis=0
        )
        for f in range(fields):
            tend = jnp.dot(PS[f], table, preferred_element_type=F32)
            for i in range(2):
                at = pl.ds(8 * (k + i), 8)
                O[f, :, at] = O[f, :, at] + tend[:, i * LANES : (i + 1) * LANES].reshape(cols, 8, LANES)

    sums = jnp.sum(Y[:, share:], axis=0) + jnp.sum(YP[:, share:], axis=0)
    cells = float(levels * east * north)
    value = jnp.broadcast_to(jnp.sqrt(jnp.maximum(sums / cells, 0.0)), (8, LANES))
    row8 = iota((8, LANES), 0)
    log = value
    for s in range(1, ITERS):
        log = jnp.where(row8 == s, pltpu.roll(value, LANES - s * fields, 1), log)
    log_ref[...] = log

    both_ends(U.at[:, pl.ds(0, 2 * HALO), body_rows], EDGE).wait_send()
    both_ends(PX, PAIR).wait_send()
    both_ends(XB.at[pl.ds(0, chips - 1)], SHARE).wait_send()
    both_ends(Y.at[pl.ds(0, chips - 1)], ALL).wait_send()
    both_ends(YP, BACK).wait_send()


def writer(O, log_ref, o_hbm, res_ref, sem):
    fields, cols, levels, north = o_hbm.shape
    chunks = north // LANES
    o_view = O.reshape(fields, cols, chunks, levels, LANES)
    for t in range(chunks):
        pltpu.make_async_copy(
            o_view.at[:, :, t], o_hbm.at[:, :, :, pl.ds(t * LANES, LANES)], sem
        ).start()
    res_ref[...] = log_ref[: res_ref.shape[0], : res_ref.shape[1]]
    pltpu.make_async_copy(O, O, sem).wait()


def solution(mesh):
    tiles = mesh.shape["gx"]
    chips = tiles // CORES

    def local(model_state, driving, mode_east, mode_north, level_class, nudge_table):
        fields, levels, cols, north = model_state.shape
        rows = levels * north // LANES
        wide, high_rows = cols + 2 * HALO, rows + 2 * PAD
        share = 16 * levels // chips
        vm = lambda *shape: pltpu.VMEM(shape, F32)
        dma = lambda *shape: pltpu.SemaphoreType.DMA(shape)
        hbm = pl.BlockSpec(memory_space=pltpu.HBM)
        smem = lambda ref: pltpu.SMEM(ref.shape, ref.dtype)
        table = nudge_table.T
        scratch = [
            smem(mode_east), smem(mode_north), smem(level_class), smem(table),
            vm(fields, wide, high_rows, LANES), vm(fields, cols, rows, LANES),
            vm(fields, ITERS - 1, wide, high_rows, LANES), pltpu.VMEM((LANES, north), jnp.bfloat16),
            vm(CORES, 32 * levels, LANES), vm(32 * levels, LANES),
            vm(chips, 2 * share, LANES), vm(chips, 2 * share, LANES),
            vm(chips, share + 1, LANES), vm(chips, share + 1, LANES), vm(CORES, 16 * levels, LANES),
            vm(ITERS * fields, 8, LANES), pltpu.VMEM((fields, 8 * cols, 2 * LANES), jnp.bfloat16),
            dma(4), dma(2, fields // 2), dma(2, fields), dma(2, 5), pltpu.SemaphoreType.REGULAR((4,)),
        ]
        turn = (0, 2, 1, 3)
        inner = pl.BlockSpec(memory_space=pltpu.VMEM)
        grid, log = pl.pallas_call(
            functools.partial(kernel, tiles),
            out_shape=(
                vm(fields, cols, rows, LANES),
                vm(8, LANES),
            ),
            in_specs=[hbm] * 6,
            out_specs=(inner, inner),
            scratch_shapes=scratch,
            compiler_params=pltpu.CompilerParams(
                collective_id=0, has_side_effects=True, vmem_limit_bytes=60 * 2**20
            ),
        )(
            model_state.transpose(turn), driving.transpose(turn),
            mode_east, mode_north, level_class, table,
        )
        nudged, log = pl.pallas_call(
            writer,
            out_shape=(
                jax.ShapeDtypeStruct((fields, cols, levels, north), F32),
                jax.ShapeDtypeStruct((ITERS, fields), F32),
            ),
            in_specs=[inner, inner],
            out_specs=(hbm, inner),
            scratch_shapes=[pltpu.SemaphoreType.DMA],
            compiler_params=pltpu.CompilerParams(vmem_limit_bytes=8 * 2**20),
        )(grid, log)
        return nudged.transpose(turn), log

    tile = P("ens", None, "gx", None)
    return jax.shard_map(
        local, mesh=mesh, in_specs=(tile, tile, P(), P(), P(), P()),
        out_specs=(tile, P("ens", None)), check_vma=False,
    )
```

```python
import functools

import jax
import jax.numpy as jnp
import numpy as np
from jax import lax
from jax.experimental import pallas as pl
from jax.experimental.pallas import tpu as pltpu
from jax.sharding import PartitionSpec as P

ITERS = 4
DIFFUSION = 0.24
CORES = 2
RING = 16
MESH = pl.DeviceIdType.MESH
HIGHEST = lax.Precision.HIGHEST
F32 = jnp.float32
LANES = 128
HALO = 4
PAD = 8
INNER_STRIPS = 3
AHEAD = 1


def iota(shape, dim):
    return lax.broadcasted_iota(jnp.int32, shape, dim)


def pick(ref, which, count):
    out = jnp.zeros(which.shape, F32)
    for i in range(count):
        out = jnp.where(which == i, ref[i].astype(F32), out)
    return out


def sine(product, period):
    turns = jnp.floor(product * (1.0 / period) + 0.5)
    x = (product - turns * period) * (np.pi / period)
    odd = turns - 2.0 * jnp.floor(turns * 0.5)
    y = x * x
    poly = 1.0 / 6227020800.0
    for c in (-1.0 / 39916800.0, 1.0 / 362880.0, -1.0 / 5040.0, 1.0 / 120.0, -1.0 / 6.0, 1.0):
        poly = poly * y + c
    return x * poly * (1.0 - 2.0 * odd)


def split(value):
    high = value.astype(jnp.bfloat16)
    return high, (value - high.astype(F32)).astype(jnp.bfloat16)


def kernel(
    tiles, u_hbm, d_hbm, me_hbm, mn_hbm, lc_hbm, nt_hbm, O, log_ref,
    me_ref, mn_ref, lc_ref, nt_ref, U, D, W, T, XD, PX, XS, XB, Y, YP, QD, ACC, PS,
    small_sem, in_sem, edge_sem, sems, heard,
):
    fields, cols, levels, north = u_hbm.shape
    kx, ky = me_ref.shape[0], mn_ref.shape[0]
    east = cols * tiles
    chips = tiles // CORES
    share = 16 * levels // chips
    chunks = north // LANES
    blocks = chunks // 2
    wide = cols + 2 * HALO
    rows = 8 * blocks
    high_rows = rows + 2 * PAD
    own = pl.ds(HALO, cols)
    g = lax.axis_index("gx")
    core = lax.rem(g, CORES)
    z = lax.rem(g // CORES, RING)
    xi = g // (CORES * RING)
    chip = g // CORES
    partner = {"gx": chip * CORES + (CORES - 1 - core)}
    right = {"gx": lax.rem(g + 1, tiles)}
    left = {"gx": lax.rem(g + tiles - 1, tiles)}
    across = chips // RING
    far_first = sorted(range(RING), key=lambda k: -min(k, RING - k))
    z_spots = [lax.rem(z + k, RING) for k in far_first]
    x_spots = [lax.rem(xi + k, across) * RING for k in range(across)]
    others = [x_spots[i] + z_spots[k] for k in range(RING) for i in range(across)]
    del others[RING * across - across]

    def peer(i):
        return {"gx": i * CORES + core}

    barrier = pltpu.get_barrier_semaphore()
    beside = [lax.rem(z + 1, RING), lax.rem(z + RING - 1, RING)]
    greeted = [partner, left, right] + [peer(x_spots[i] + z) for i in range(1, across)]
    greeted += [peer(x + there) for there in beside for x in x_spots]
    for who in greeted:
        pl.semaphore_signal(barrier, inc=1, device_id=who, device_id_type=MESH)
    rounds = [1 << i for i in range(8) if 4 << i <= RING]

    def hear(i):
        if i < len(rounds):
            pl.semaphore_wait(heard.at[i], 2)

    def tell(i):
        if i < len(rounds):
            for there in (lax.rem(z + rounds[i], RING), lax.rem(z + RING - rounds[i], RING)):
                pl.semaphore_signal(
                    heard.at[i], inc=1, device_id=peer(xi * RING + there), device_id_type=MESH
                )

    u_view = U.reshape(fields, wide, high_rows // levels, levels, LANES)
    d_view = D.reshape(fields, cols, chunks, levels, LANES)
    skip = PAD // levels
    small = []
    for i, (hbm, ref) in enumerate(((me_hbm, me_ref), (mn_hbm, mn_ref), (lc_hbm, lc_ref), (nt_hbm, nt_ref))):
        small.append(pltpu.make_async_copy(hbm, ref, small_sem.at[i]))
        small[-1].start()
    for h in range(0, fields, 2):
        two = pl.ds(h, 2)
        for i in range(2):
            for t in range(chunks):
                hbm, dst = (
                    (u_hbm, u_view.at[two, own, skip + t]) if i == 0 else (d_hbm, d_view.at[two, :, t])
                )
                pltpu.make_async_copy(
                    hbm.at[two, :, :, pl.ds(t * LANES, LANES)], dst, in_sem.at[i, h // 2]
                ).start()

    def loaded(i, h):
        two = pl.ds(h, 2)
        ref = U.at[two, own, pl.ds(PAD, rows)] if i == 0 else D.at[two]
        pltpu.make_async_copy(ref, ref, in_sem.at[i, h // 2]).wait()

    for copy in small:
        copy.wait()
    row32 = iota((32, LANES), 0)
    lane32 = iota((32, LANES), 1)
    modes_n = pick(mn_ref, row32, ky)
    for c in range(chunks):
        place = (lane32 + (c * LANES + 1)).astype(F32)
        high, low = split(sine(modes_n * place, float(north + 1)))
        at = pl.ds(c * LANES, LANES)
        both = jnp.concatenate([high, low], axis=0)
        T[0:64, at] = both
        T[64:128, at] = both
    first = g * cols
    count = 8 * cols
    grid_rows = 8 * ((count + LANES - 1) // LANES) * (LANES // 8)
    row_m, lane_m = iota((LANES, grid_rows), 0), iota((LANES, grid_rows), 1)
    mode_m = pick(me_ref, iota((LANES, LANES), 0) % 32, kx)
    mode_m = jnp.concatenate([mode_m] * (grid_rows // LANES), axis=1)
    to_modes = jnp.where(
        (lane_m < count) & (row_m // 32 == lane_m % 4),
        sine(mode_m * (lane_m // 8 + first + 1).astype(F32), float(east + 1)), 0.0,
    )
    row_g, lane_g = iota((count, LANES), 0), iota((count, LANES), 1)
    mode_g = jnp.concatenate([pick(me_ref, iota((8, LANES), 1) % 32, kx)] * cols, axis=0)
    to_grid = jnp.where(
        row_g % 4 == lane_g // 32,
        sine(mode_g * (row_g // 8 + first + 1).astype(F32), float(east + 1)), 0.0,
    )
    row16 = iota((16, LANES), 0)
    lane16 = iota((16, LANES), 1)
    f_low = 2 * core
    my_class = lc_ref[(chip * share) // 16]
    w_low, w_up = nt_ref[f_low, my_class], nt_ref[f_low + 1, my_class]

    def constants(top, count):
        lane = iota((count, LANES), 1)
        a = iota((count, LANES), 0) + top + jnp.where(lane >= 64, 16, 0)
        half_e = sine(pick(me_ref, a, kx), 2.0 * (east + 1))
        half_n = sine(pick(mn_ref, lane % 32, ky), 2.0 * (north + 1))
        fade = (4.0 * DIFFUSION) * (half_e * half_e + half_n * half_n)
        return fade, jnp.where(lane % 64 >= 32, w_up, w_low)

    def substeps(fade, w, r, d):
        lam = 1.0 - fade
        t = jnp.zeros_like(r)
        v = r
        out = []
        for _ in range(ITERS):
            t = lam * t + w * r
            r = (lam - w) * r + fade * d
            v = lam * v + fade * d
            out.append((t, r, v))
        return out

    my_modes = constants(lax.rem(chip * share, 16), share)

    pl.semaphore_wait(barrier, len(greeted))
    tell(0)

    def send(src, dst, phase, who, recv_sem=None):
        pltpu.make_async_remote_copy(
            src_ref=src, dst_ref=dst, send_sem=sems.at[0, phase],
            recv_sem=sems.at[1, phase] if recv_sem is None else recv_sem,
            device_id=who, device_id_type=MESH,
        ).start()

    def both_ends(ref, phase, recv_sem=None):
        return pltpu.make_async_remote_copy(
            src_ref=ref, dst_ref=ref, send_sem=sems.at[0, phase],
            recv_sem=sems.at[1, phase] if recv_sem is None else recv_sem,
            device_id=right, device_id_type=MESH,
        )

    EDGE, PAIR, SHARE, ALL, BACK = range(5)
    body_rows = pl.ds(PAD, rows)
    west, inner_west = pl.ds(0, HALO), pl.ds(HALO, HALO)
    inner_east, east_edge = pl.ds(cols, HALO), pl.ds(HALO + cols, HALO)

    def send_edges(f):
        send(U.at[f, inner_east, body_rows], U.at[f, west, body_rows], EDGE, right, edge_sem.at[0, f])
        send(U.at[f, inner_west, body_rows], U.at[f, east_edge, body_rows], EDGE, left, edge_sem.at[1, f])

    norm = 4.0 / ((east + 1) * (north + 1))
    odd_chunk = row_g % 8 >= 4
    contract_lanes = (((1,), (1,)), ((), ()))
    for h in range(0, fields, 2):
        loaded(0, h)
        for f in range(h, min(h + 2, fields - 1)):
            send_edges(f)
        hear(h // 2)
        tell(h // 2 + 1)
        loaded(1, h)
        acc_r = acc_d = None
        held = []
        for k in range(blocks):
            at = pl.ds(8 * k, 8)
            d = D[h : h + 2, :, at]
            r = d - U[h : h + 2, own, pl.ds(PAD + 8 * k, 8)]
            high, low = split(r.reshape(2 * count, LANES))
            table = jnp.concatenate(
                [T[0:64, pl.ds((2 * k + p) * LANES, LANES)] for p in range(2)], axis=0
            )
            out = lax.dot_general(
                jnp.concatenate([high, low], axis=1), jnp.concatenate([table, table], axis=1),
                contract_lanes, preferred_element_type=F32,
            )
            acc_r = out if acc_r is None else acc_r + out
            held.append((d.reshape(2 * count, LANES).astype(jnp.bfloat16), table))
            if len(held) == 2:
                out = lax.dot_general(
                    jnp.concatenate([held[0][0], held[1][0]], axis=1),
                    jnp.concatenate([held[0][1], held[1][1]], axis=1),
                    contract_lanes, preferred_element_type=F32,
                )
                acc_d = out if acc_d is None else acc_d + out
                held = []
        mix = jnp.zeros((count, LANES), F32)
        for i, acc in enumerate((acc_r, acc_d)):
            acc = acc + pltpu.roll(acc, 32, 1)
            for j in range(2):
                mine = acc[j * count : (j + 1) * count]
                slot = 2 * i + j
                even, odd = ((slot - 1) % 4) * 32, ((slot + 1) % 4) * 32
                even = pltpu.roll(mine, even, 1) if even else mine
                odd = pltpu.roll(mine, odd, 1) if odd else mine
                mix = jnp.where(lane_g // 32 == slot, jnp.where(odd_chunk, odd, even), mix)
        if grid_rows > count:
            mix = jnp.concatenate([mix, jnp.zeros((grid_rows - count, LANES), F32)], axis=0)
        modal = norm * jnp.dot(to_modes, mix, precision=HIGHEST, preferred_element_type=F32)
        turned = pltpu.roll(modal, 64, 1)
        for l in range(levels):
            upper_a, lower_a = slice(32 * l, 32 * l + 16), slice(32 * l + 16, 32 * l + 32)
            XD[h // 2, 32 * l : 32 * l + 16] = jnp.where(lane16 < 64, modal[upper_a], turned[lower_a])
            XD[h // 2, 32 * l + 16 : 32 * l + 32] = jnp.where(lane16 < 64, turned[upper_a], modal[lower_a])

    def outside(ref, *at):
        hollow = jnp.zeros((HALO, rows, LANES), F32)

        @pl.when(g == 0)
        def _():
            ref[(*at, pl.ds(0, HALO), body_rows)] = hollow

        @pl.when(g == tiles - 1)
        def _():
            ref[(*at, pl.ds(HALO + cols, HALO), body_rows)] = hollow

    def update(f, s, bounds, strips):
        src = U.at[f] if s == 0 else W.at[f, s - 1]
        acc = jnp.zeros((8, LANES), F32)
        cuts = []
        for lo, hi in bounds:
            cuts += [(lo + (hi - lo) * i // strips, lo + (hi - lo) * (i + 1) // strips) for i in range(strips)]
        for k in range(blocks):
            r = PAD + 8 * k
            for x0, x1 in cuts:
                near = src[x0 - 1 : x1 + 1, r : r + 8]
                cur = near[1:-1]
                lane = iota((x1 - x0, 8, LANES), 2)
                below = src[x0:x1, r - 4 : r + 4]
                above = src[x0:x1, r + 4 : r + 12]
                south = pltpu.roll(jnp.where(lane == LANES - 1, below, cur), 1, 2)
                north_of = pltpu.roll(jnp.where(lane == 0, above, cur), LANES - 1, 2)
                around = (near[:-2] + near[2:]) + (south + north_of)
                new = (1.0 - 4.0 * DIFFUSION) * cur + DIFFUSION * around
                if s + 1 < ITERS:
                    W[f, s, x0:x1, r : r + 8] = new
                y0, y1 = max(x0, HALO), min(x1, HALO + cols)
                if y0 >= y1:
                    continue
                at = slice(y0 - HALO, y1 - HALO)
                new = new[y0 - x0 : y1 - x0]
                if s + 1 == ITERS:
                    O[f, at, 8 * k : 8 * k + 8] = new
                gap = D[f, at, 8 * k : 8 * k + 8] - new
                acc = acc + jnp.sum(gap * gap, axis=0)
        return acc

    def diffuse_inner(f):
        for s in range(ITERS):
            ACC[s * fields + f] = update(f, s, [(HALO + 1 + s, HALO + cols - 1 - s)], INNER_STRIPS)

    def diffuse_edges(f):
        both_ends(U.at[f, west, body_rows], EDGE, edge_sem.at[0, f]).wait_recv()
        both_ends(U.at[f, east_edge, body_rows], EDGE, edge_sem.at[1, f]).wait_recv()
        outside(U, f)
        for s in range(ITERS):
            spans = [(s + 1, HALO + 1 + s), (HALO + cols - 1 - s, wide - 1 - s)]
            acc = update(f, s, spans, 1)
            ACC[s * fields + f] = ACC[s * fields + f] + acc
            if s + 1 < ITERS:
                outside(W, f, s)

    send(XD.at[CORES - 1 - core], PX, PAIR, partner)
    rim = jnp.zeros((wide, PAD, LANES), F32)
    for f in range(fields):
        for ref in [U.at[f]] + [W.at[f, s] for s in range(ITERS - 1)]:
            ref[:, 0:PAD] = rim
            ref[:, PAD + rows : high_rows] = rim
    lax.fori_loop(0, AHEAD, lambda f, c: (diffuse_inner(f), c)[1], 0)
    both_ends(PX, PAIR).wait_recv()
    total = XD[core] + PX[...]
    for i in range(chips):
        l, top = (i * share) // 16, (i * share) % 16
        XS[i, :share] = total[32 * l + top : 32 * l + top + share]
        XS[i, share:] = total[32 * l + 16 + top : 32 * l + 16 + top + share]
    for i in range(2, len(rounds)):
        hear(i)
        tell(i + 1)
    for i in others:
        send(XS.at[i], XB.at[chip], SHARE, peer(i))
    send_edges(fields - 1)
    XB[chip] = XS[chip]
    lax.fori_loop(AHEAD, fields, lambda f, c: (diffuse_inner(f), c)[1], 0)
    lax.fori_loop(0, fields, lambda f, c: (diffuse_edges(f), c)[1], 0)

    both_ends(XB.at[pl.ds(0, chips - 1)], SHARE).wait_recv()
    shares = jnp.sum(XB[...], axis=0)
    r_sum, d_sum = shares[:share], shares[share:]
    energy = jnp.zeros((16, LANES), F32)
    weight = -0.25 * (east + 1.0) * (north + 1.0)
    my_field = jnp.where(lane16 % 64 >= 32, f_low + 1, f_low)
    course = substeps(*my_modes, r_sum, d_sum)
    for s, (t, r, v) in enumerate(course):
        part = jnp.sum(weight * t * (r + v), axis=0, keepdims=True)
        energy = jnp.where(row16 == s * fields + my_field, part, energy)
    for i in range(ITERS * fields):
        energy = energy + jnp.where(row16 == i, jnp.sum(ACC[i], axis=0, keepdims=True), 0.0)
    energy = jnp.sum(energy, axis=1, keepdims=True)
    Y[chip, :share] = course[-1][0]
    Y[chip, share:] = jnp.sum(jnp.where(row16 == lane16, energy, 0.0), axis=0, keepdims=True)
    for i in others:
        send(Y.at[chip], Y.at[chip], ALL, peer(i))
    both_ends(Y.at[pl.ds(0, chips - 1)], ALL).wait_recv()
    send(Y, YP, BACK, partner)
    for i in range(chips):
        QD[core, i * share : (i + 1) * share] = Y[i, :share]

    both_ends(YP, BACK).wait_recv()
    for i in range(chips):
        QD[CORES - 1 - core, i * share : (i + 1) * share] = YP[i, :share]
    for h in range(fields // 2):
        parts = []
        for l in range(levels):
            packed = QD[h, 16 * l : 16 * l + 16]
            parts += [packed, pltpu.roll(packed, 64, 1)]
        modal = jnp.dot(
            to_grid, jnp.concatenate(parts, axis=0), precision=HIGHEST, preferred_element_type=F32
        )
        for k in range(2):
            mine = jnp.where(lane_g // 32 == k, modal, 0.0)
            mine = mine + pltpu.roll(mine, 32, 1)
            mine = mine + pltpu.roll(mine, 64, 1)
            high = mine.astype(jnp.bfloat16).astype(F32)
            mine = jnp.where(lane_g < 64, high, mine - high)
            PS[2 * h + k] = jnp.concatenate(
                [jnp.where(odd_chunk, 0.0, mine), jnp.where(odd_chunk, mine, 0.0)], axis=1
            ).astype(jnp.bfloat16)
    for k in range(0, blocks, 2):
        quad = [T[:, pl.ds((2 * k + i) * LANES, LANES)] for i in range(4)]
        table = jnp.concatenate(
            [jnp.concatenate(quad[0::2], axis=1), jnp.concatenate(quad[1::2], axis=1)], axis=0
        )
        for f in range(fields):
            tend = jnp.dot(PS[f], table, preferred_element_type=F32)
            for i in range(2):
                at = pl.ds(8 * (k + i), 8)
                O[f, :, at] = O[f, :, at] + tend[:, i * LANES : (i + 1) * LANES].reshape(cols, 8, LANES)

    sums = jnp.sum(Y[:, share:], axis=0) + jnp.sum(YP[:, share:], axis=0)
    cells = float(levels * east * north)
    value = jnp.broadcast_to(jnp.sqrt(jnp.maximum(sums / cells, 0.0)), (8, LANES))
    row8 = iota((8, LANES), 0)
    log = value
    for s in range(1, ITERS):
        log = jnp.where(row8 == s, pltpu.roll(value, LANES - s * fields, 1), log)
    log_ref[...] = log

    both_ends(U.at[:, pl.ds(0, 2 * HALO), body_rows], EDGE).wait_send()
    both_ends(PX, PAIR).wait_send()
    both_ends(XB.at[pl.ds(0, chips - 1)], SHARE).wait_send()
    both_ends(Y.at[pl.ds(0, chips - 1)], ALL).wait_send()
    both_ends(YP, BACK).wait_send()


def writer(O, log_ref, o_hbm, res_ref, sem):
    fields, cols, levels, north = o_hbm.shape
    chunks = north // LANES
    o_view = O.reshape(fields, cols, chunks, levels, LANES)
    for t in range(chunks):
        pltpu.make_async_copy(
            o_view.at[:, :, t], o_hbm.at[:, :, :, pl.ds(t * LANES, LANES)], sem
        ).start()
    res_ref[...] = log_ref[: res_ref.shape[0], : res_ref.shape[1]]
    pltpu.make_async_copy(O, O, sem).wait()


def solution(mesh):
    tiles = mesh.shape["gx"]
    chips = tiles // CORES

    def local(model_state, driving, mode_east, mode_north, level_class, nudge_table):
        fields, levels, cols, north = model_state.shape
        rows = levels * north // LANES
        wide, high_rows = cols + 2 * HALO, rows + 2 * PAD
        share = 16 * levels // chips
        vm = lambda *shape: pltpu.VMEM(shape, F32)
        dma = lambda *shape: pltpu.SemaphoreType.DMA(shape)
        hbm = pl.BlockSpec(memory_space=pltpu.HBM)
        smem = lambda ref: pltpu.SMEM(ref.shape, ref.dtype)
        table = nudge_table.T
        scratch = [
            smem(mode_east), smem(mode_north), smem(level_class), smem(table),
            vm(fields, wide, high_rows, LANES), vm(fields, cols, rows, LANES),
            vm(fields, ITERS - 1, wide, high_rows, LANES), pltpu.VMEM((LANES, north), jnp.bfloat16),
            vm(CORES, 32 * levels, LANES), vm(32 * levels, LANES),
            vm(chips, 2 * share, LANES), vm(chips, 2 * share, LANES),
            vm(chips, share + 1, LANES), vm(chips, share + 1, LANES), vm(CORES, 16 * levels, LANES),
            vm(ITERS * fields, 8, LANES), pltpu.VMEM((fields, 8 * cols, 2 * LANES), jnp.bfloat16),
            dma(4), dma(2, fields // 2), dma(2, fields), dma(2, 5), pltpu.SemaphoreType.REGULAR((4,)),
        ]
        turn = (0, 2, 1, 3)
        inner = pl.BlockSpec(memory_space=pltpu.VMEM)
        grid, log = pl.pallas_call(
            functools.partial(kernel, tiles),
            out_shape=(
                vm(fields, cols, rows, LANES),
                vm(8, LANES),
            ),
            in_specs=[hbm] * 6,
            out_specs=(inner, inner),
            scratch_shapes=scratch,
            compiler_params=pltpu.CompilerParams(
                collective_id=0, has_side_effects=True, vmem_limit_bytes=60 * 2**20
            ),
        )(
            model_state.transpose(turn), driving.transpose(turn),
            mode_east, mode_north, level_class, table,
        )
        nudged, log = pl.pallas_call(
            writer,
            out_shape=(
                jax.ShapeDtypeStruct((fields, cols, levels, north), F32),
                jax.ShapeDtypeStruct((ITERS, fields), F32),
            ),
            in_specs=[inner, inner],
            out_specs=(hbm, inner),
            scratch_shapes=[pltpu.SemaphoreType.DMA],
            compiler_params=pltpu.CompilerParams(vmem_limit_bytes=8 * 2**20),
        )(grid, log)
        return nudged.transpose(turn), log

    tile = P("ens", None, "gx", None)
    return jax.shard_map(
        local, mesh=mesh, in_specs=(tile, tile, P(), P(), P(), P()),
        out_specs=(tile, P("ens", None)), check_vma=False,
    )
```

```python
import functools

import jax
import jax.numpy as jnp
import numpy as np
from jax import lax
from jax.experimental import pallas as pl
from jax.experimental.pallas import tpu as pltpu
from jax.sharding import PartitionSpec as P

ITERS = 4
DIFFUSION = 0.24
CORES = 2
RING = 16
MESH = pl.DeviceIdType.MESH
HIGHEST = lax.Precision.HIGHEST
F32 = jnp.float32
LANES = 128
HALO = 4
PAD = 8
INNER_STRIPS = 3
AHEAD = 1


def iota(shape, dim):
    return lax.broadcasted_iota(jnp.int32, shape, dim)


def pick(ref, which, count):
    out = jnp.zeros(which.shape, F32)
    for i in range(count):
        out = jnp.where(which == i, ref[i].astype(F32), out)
    return out


def sine(product, period):
    turns = jnp.floor(product * (1.0 / period) + 0.5)
    x = (product - turns * period) * (np.pi / period)
    odd = turns - 2.0 * jnp.floor(turns * 0.5)
    y = x * x
    poly = 1.0 / 6227020800.0
    for c in (-1.0 / 39916800.0, 1.0 / 362880.0, -1.0 / 5040.0, 1.0 / 120.0, -1.0 / 6.0, 1.0):
        poly = poly * y + c
    return x * poly * (1.0 - 2.0 * odd)


def split(value):
    high = value.astype(jnp.bfloat16)
    return high, (value - high.astype(F32)).astype(jnp.bfloat16)


def kernel(
    tiles, u_hbm, d_hbm, me_hbm, mn_hbm, lc_hbm, nt_hbm, O, log_ref,
    me_ref, mn_ref, lc_ref, nt_ref, U, D, W, T, XD, PX, XS, XB, Y, YP, QD, ACC, PS,
    small_sem, in_sem, edge_sem, sems, heard,
):
    fields, cols, levels, north = u_hbm.shape
    kx, ky = me_ref.shape[0], mn_ref.shape[0]
    east = cols * tiles
    chips = tiles // CORES
    share = 16 * levels // chips
    chunks = north // LANES
    blocks = chunks // 2
    wide = cols + 2 * HALO
    rows = 8 * blocks
    high_rows = rows + 2 * PAD
    own = pl.ds(HALO, cols)
    g = lax.axis_index("gx")
    core = lax.rem(g, CORES)
    z = lax.rem(g // CORES, RING)
    xi = g // (CORES * RING)
    chip = g // CORES
    partner = {"gx": chip * CORES + (CORES - 1 - core)}
    right = {"gx": lax.rem(g + 1, tiles)}
    left = {"gx": lax.rem(g + tiles - 1, tiles)}
    across = chips // RING
    far_first = sorted(range(RING), key=lambda k: -min(k, RING - k))
    z_spots = [lax.rem(z + k, RING) for k in far_first]
    x_spots = [lax.rem(xi + k, across) * RING for k in range(across)]
    others = [x_spots[i] + z_spots[k] for k in range(RING) for i in range(across)]
    del others[RING * across - across]

    def peer(i):
        return {"gx": i * CORES + core}

    barrier = pltpu.get_barrier_semaphore()
    beside = [lax.rem(z + 1, RING), lax.rem(z + RING - 1, RING)]
    greeted = [partner, left, right] + [peer(x_spots[i] + z) for i in range(1, across)]
    greeted += [peer(x + there) for there in beside for x in x_spots]
    for who in greeted:
        pl.semaphore_signal(barrier, inc=1, device_id=who, device_id_type=MESH)
    rounds = [1 << i for i in range(8) if 4 << i <= RING]

    def hear(i):
        if i < len(rounds):
            pl.semaphore_wait(heard.at[i], 2)

    def tell(i):
        if i < len(rounds):
            for there in (lax.rem(z + rounds[i], RING), lax.rem(z + RING - rounds[i], RING)):
                pl.semaphore_signal(
                    heard.at[i], inc=1, device_id=peer(xi * RING + there), device_id_type=MESH
                )

    u_view = U.reshape(fields, wide, high_rows // levels, levels, LANES)
    d_view = D.reshape(fields, cols, chunks, levels, LANES)
    skip = PAD // levels
    small = []
    for i, (hbm, ref) in enumerate(((me_hbm, me_ref), (mn_hbm, mn_ref), (lc_hbm, lc_ref), (nt_hbm, nt_ref))):
        small.append(pltpu.make_async_copy(hbm, ref, small_sem.at[i]))
        small[-1].start()
    for h in range(0, fields, 2):
        two = pl.ds(h, 2)
        for i in range(2):
            for t in range(chunks):
                hbm, dst = (
                    (u_hbm, u_view.at[two, own, skip + t]) if i == 0 else (d_hbm, d_view.at[two, :, t])
                )
                pltpu.make_async_copy(
                    hbm.at[two, :, :, pl.ds(t * LANES, LANES)], dst, in_sem.at[i, h // 2]
                ).start()

    def loaded(i, h):
        two = pl.ds(h, 2)
        ref = U.at[two, own, pl.ds(PAD, rows)] if i == 0 else D.at[two]
        pltpu.make_async_copy(ref, ref, in_sem.at[i, h // 2]).wait()

    for copy in small:
        copy.wait()
    row32 = iota((32, LANES), 0)
    lane32 = iota((32, LANES), 1)
    modes_n = pick(mn_ref, row32, ky)
    for c in range(chunks):
        place = (lane32 + (c * LANES + 1)).astype(F32)
        high, low = split(sine(modes_n * place, float(north + 1)))
        at = pl.ds(c * LANES, LANES)
        both = jnp.concatenate([high, low], axis=0)
        T[0:64, at] = both
        T[64:128, at] = both
    first = g * cols
    count = 8 * cols
    grid_rows = 8 * ((count + LANES - 1) // LANES) * (LANES // 8)
    row_m, lane_m = iota((LANES, grid_rows), 0), iota((LANES, grid_rows), 1)
    mode_m = pick(me_ref, iota((LANES, LANES), 0) % 32, kx)
    mode_m = jnp.concatenate([mode_m] * (grid_rows // LANES), axis=1)
    to_modes = jnp.where(
        (lane_m < count) & (row_m // 32 == lane_m % 4),
        sine(mode_m * (lane_m // 8 + first + 1).astype(F32), float(east + 1)), 0.0,
    )
    row_g, lane_g = iota((count, LANES), 0), iota((count, LANES), 1)
    mode_g = jnp.concatenate([pick(me_ref, iota((8, LANES), 1) % 32, kx)] * cols, axis=0)
    to_grid = jnp.where(
        row_g % 4 == lane_g // 32,
        sine(mode_g * (row_g // 8 + first + 1).astype(F32), float(east + 1)), 0.0,
    )
    row16 = iota((16, LANES), 0)
    lane16 = iota((16, LANES), 1)
    f_low = 2 * core
    my_class = lc_ref[(chip * share) // 16]
    w_low, w_up = nt_ref[f_low, my_class], nt_ref[f_low + 1, my_class]

    def constants(top, count):
        lane = iota((count, LANES), 1)
        a = iota((count, LANES), 0) + top + jnp.where(lane >= 64, 16, 0)
        half_e = sine(pick(me_ref, a, kx), 2.0 * (east + 1))
        half_n = sine(pick(mn_ref, lane % 32, ky), 2.0 * (north + 1))
        fade = (4.0 * DIFFUSION) * (half_e * half_e + half_n * half_n)
        return fade, jnp.where(lane % 64 >= 32, w_up, w_low)

    def substeps(fade, w, r, d):
        lam = 1.0 - fade
        t = jnp.zeros_like(r)
        v = r
        out = []
        for _ in range(ITERS):
            t = lam * t + w * r
            r = (lam - w) * r + fade * d
            v = lam * v + fade * d
            out.append((t, r, v))
        return out

    my_modes = constants(lax.rem(chip * share, 16), share)

    pl.semaphore_wait(barrier, len(greeted))
    tell(0)

    def send(src, dst, phase, who, recv_sem=None):
        pltpu.make_async_remote_copy(
            src_ref=src, dst_ref=dst, send_sem=sems.at[0, phase],
            recv_sem=sems.at[1, phase] if recv_sem is None else recv_sem,
            device_id=who, device_id_type=MESH,
        ).start()

    def both_ends(ref, phase, recv_sem=None):
        return pltpu.make_async_remote_copy(
            src_ref=ref, dst_ref=ref, send_sem=sems.at[0, phase],
            recv_sem=sems.at[1, phase] if recv_sem is None else recv_sem,
            device_id=right, device_id_type=MESH,
        )

    EDGE, PAIR, SHARE, ALL, BACK = range(5)
    body_rows = pl.ds(PAD, rows)
    west, inner_west = pl.ds(0, HALO), pl.ds(HALO, HALO)
    inner_east, east_edge = pl.ds(cols, HALO), pl.ds(HALO + cols, HALO)

    def send_edges(f):
        send(U.at[f, inner_east, body_rows], U.at[f, west, body_rows], EDGE, right, edge_sem.at[0, f])
        send(U.at[f, inner_west, body_rows], U.at[f, east_edge, body_rows], EDGE, left, edge_sem.at[1, f])

    def outside(ref, *at):
        hollow = jnp.zeros((HALO, rows, LANES), F32)

        @pl.when(g == 0)
        def _():
            ref[(*at, pl.ds(0, HALO), body_rows)] = hollow

        @pl.when(g == tiles - 1)
        def _():
            ref[(*at, pl.ds(HALO + cols, HALO), body_rows)] = hollow

    def update(f, s, bounds, strips):
        src = U.at[f] if s == 0 else W.at[f, s - 1]
        acc = jnp.zeros((8, LANES), F32)
        cuts = []
        for lo, hi in bounds:
            cuts += [(lo + (hi - lo) * i // strips, lo + (hi - lo) * (i + 1) // strips) for i in range(strips)]
        for k in range(blocks):
            r = PAD + 8 * k
            for x0, x1 in cuts:
                near = src[x0 - 1 : x1 + 1, r : r + 8]
                cur = near[1:-1]
                lane = iota((x1 - x0, 8, LANES), 2)
                below = src[x0:x1, r - 4 : r + 4]
                above = src[x0:x1, r + 4 : r + 12]
                south = pltpu.roll(jnp.where(lane == LANES - 1, below, cur), 1, 2)
                north_of = pltpu.roll(jnp.where(lane == 0, above, cur), LANES - 1, 2)
                around = (near[:-2] + near[2:]) + (south + north_of)
                new = (1.0 - 4.0 * DIFFUSION) * cur + DIFFUSION * around
                if s + 1 < ITERS:
                    W[f, s, x0:x1, r : r + 8] = new
                y0, y1 = max(x0, HALO), min(x1, HALO + cols)
                if y0 >= y1:
                    continue
                at = slice(y0 - HALO, y1 - HALO)
                new = new[y0 - x0 : y1 - x0]
                if s + 1 == ITERS:
                    O[f, at, 8 * k : 8 * k + 8] = new
                gap = D[f, at, 8 * k : 8 * k + 8] - new
                acc = acc + jnp.sum(gap * gap, axis=0)
        return acc

    def diffuse_inner(f):
        for s in range(ITERS):
            ACC[s * fields + f] = update(f, s, [(HALO + 1 + s, HALO + cols - 1 - s)], INNER_STRIPS)

    def diffuse_edges(f):
        both_ends(U.at[f, west, body_rows], EDGE, edge_sem.at[0, f]).wait_recv()
        both_ends(U.at[f, east_edge, body_rows], EDGE, edge_sem.at[1, f]).wait_recv()
        outside(U, f)
        for s in range(ITERS):
            spans = [(s + 1, HALO + 1 + s), (HALO + cols - 1 - s, wide - 1 - s)]
            acc = update(f, s, spans, 1)
            ACC[s * fields + f] = ACC[s * fields + f] + acc
            if s + 1 < ITERS:
                outside(W, f, s)

    norm = 4.0 / ((east + 1) * (north + 1))
    odd_chunk = row_g % 8 >= 4
    contract_lanes = (((1,), (1,)), ((), ()))
    for h in range(0, fields, 2):
        loaded(0, h)
        for f in range(h, min(h + 2, fields - 1)):
            send_edges(f)
        loaded(1, h)
        if h == 0:
            rim = jnp.zeros((wide, PAD, LANES), F32)
            for f in range(fields):
                for ref in [U.at[f]] + [W.at[f, s] for s in range(ITERS - 1)]:
                    ref[:, 0:PAD] = rim
                    ref[:, PAD + rows : high_rows] = rim
            lax.fori_loop(0, AHEAD, lambda f, c: (diffuse_inner(f), c)[1], 0)
        hear(h // 2)
        tell(h // 2 + 1)
        acc_r = acc_d = None
        held = []
        for k in range(blocks):
            at = pl.ds(8 * k, 8)
            d = D[h : h + 2, :, at]
            r = d - U[h : h + 2, own, pl.ds(PAD + 8 * k, 8)]
            high, low = split(r.reshape(2 * count, LANES))
            table = jnp.concatenate(
                [T[0:64, pl.ds((2 * k + p) * LANES, LANES)] for p in range(2)], axis=0
            )
            out = lax.dot_general(
                jnp.concatenate([high, low], axis=1), jnp.concatenate([table, table], axis=1),
                contract_lanes, preferred_element_type=F32,
            )
            acc_r = out if acc_r is None else acc_r + out
            held.append((d.reshape(2 * count, LANES).astype(jnp.bfloat16), table))
            if len(held) == 2:
                out = lax.dot_general(
                    jnp.concatenate([held[0][0], held[1][0]], axis=1),
                    jnp.concatenate([held[0][1], held[1][1]], axis=1),
                    contract_lanes, preferred_element_type=F32,
                )
                acc_d = out if acc_d is None else acc_d + out
                held = []
        mix = jnp.zeros((count, LANES), F32)
        for i, acc in enumerate((acc_r, acc_d)):
            acc = acc + pltpu.roll(acc, 32, 1)
            for j in range(2):
                mine = acc[j * count : (j + 1) * count]
                slot = 2 * i + j
                even, odd = ((slot - 1) % 4) * 32, ((slot + 1) % 4) * 32
                even = pltpu.roll(mine, even, 1) if even else mine
                odd = pltpu.roll(mine, odd, 1) if odd else mine
                mix = jnp.where(lane_g // 32 == slot, jnp.where(odd_chunk, odd, even), mix)
        if grid_rows > count:
            mix = jnp.concatenate([mix, jnp.zeros((grid_rows - count, LANES), F32)], axis=0)
        modal = norm * jnp.dot(to_modes, mix, precision=HIGHEST, preferred_element_type=F32)
        turned = pltpu.roll(modal, 64, 1)
        for l in range(levels):
            upper_a, lower_a = slice(32 * l, 32 * l + 16), slice(32 * l + 16, 32 * l + 32)
            XD[h // 2, 32 * l : 32 * l + 16] = jnp.where(lane16 < 64, modal[upper_a], turned[lower_a])
            XD[h // 2, 32 * l + 16 : 32 * l + 32] = jnp.where(lane16 < 64, turned[upper_a], modal[lower_a])

    send(XD.at[CORES - 1 - core], PX, PAIR, partner)
    both_ends(PX, PAIR).wait_recv()
    total = XD[core] + PX[...]
    for i in range(chips):
        l, top = (i * share) // 16, (i * share) % 16
        XS[i, :share] = total[32 * l + top : 32 * l + top + share]
        XS[i, share:] = total[32 * l + 16 + top : 32 * l + 16 + top + share]
    for i in range(2, len(rounds)):
        hear(i)
        tell(i + 1)
    for i in others:
        send(XS.at[i], XB.at[chip], SHARE, peer(i))
    send_edges(fields - 1)
    XB[chip] = XS[chip]
    lax.fori_loop(AHEAD, fields, lambda f, c: (diffuse_inner(f), c)[1], 0)
    lax.fori_loop(0, fields, lambda f, c: (diffuse_edges(f), c)[1], 0)

    both_ends(XB.at[pl.ds(0, chips - 1)], SHARE).wait_recv()
    shares = jnp.sum(XB[...], axis=0)
    r_sum, d_sum = shares[:share], shares[share:]
    energy = jnp.zeros((16, LANES), F32)
    weight = -0.25 * (east + 1.0) * (north + 1.0)
    my_field = jnp.where(lane16 % 64 >= 32, f_low + 1, f_low)
    course = substeps(*my_modes, r_sum, d_sum)
    for s, (t, r, v) in enumerate(course):
        part = jnp.sum(weight * t * (r + v), axis=0, keepdims=True)
        energy = jnp.where(row16 == s * fields + my_field, part, energy)
    for i in range(ITERS * fields):
        energy = energy + jnp.where(row16 == i, jnp.sum(ACC[i], axis=0, keepdims=True), 0.0)
    energy = jnp.sum(energy, axis=1, keepdims=True)
    Y[chip, :share] = course[-1][0]
    Y[chip, share:] = jnp.sum(jnp.where(row16 == lane16, energy, 0.0), axis=0, keepdims=True)
    for i in others:
        send(Y.at[chip], Y.at[chip], ALL, peer(i))
    both_ends(Y.at[pl.ds(0, chips - 1)], ALL).wait_recv()
    send(Y, YP, BACK, partner)
    for i in range(chips):
        QD[core, i * share : (i + 1) * share] = Y[i, :share]

    both_ends(YP, BACK).wait_recv()
    for i in range(chips):
        QD[CORES - 1 - core, i * share : (i + 1) * share] = YP[i, :share]
    for h in range(fields // 2):
        parts = []
        for l in range(levels):
            packed = QD[h, 16 * l : 16 * l + 16]
            parts += [packed, pltpu.roll(packed, 64, 1)]
        modal = jnp.dot(
            to_grid, jnp.concatenate(parts, axis=0), precision=HIGHEST, preferred_element_type=F32
        )
        for k in range(2):
            mine = jnp.where(lane_g // 32 == k, modal, 0.0)
            mine = mine + pltpu.roll(mine, 32, 1)
            mine = mine + pltpu.roll(mine, 64, 1)
            high = mine.astype(jnp.bfloat16).astype(F32)
            mine = jnp.where(lane_g < 64, high, mine - high)
            PS[2 * h + k] = jnp.concatenate(
                [jnp.where(odd_chunk, 0.0, mine), jnp.where(odd_chunk, mine, 0.0)], axis=1
            ).astype(jnp.bfloat16)
    for k in range(0, blocks, 2):
        quad = [T[:, pl.ds((2 * k + i) * LANES, LANES)] for i in range(4)]
        table = jnp.concatenate(
            [jnp.concatenate(quad[0::2], axis=1), jnp.concatenate(quad[1::2], axis=1)], axis=0
        )
        for f in range(fields):
            tend = jnp.dot(PS[f], table, preferred_element_type=F32)
            for i in range(2):
                at = pl.ds(8 * (k + i), 8)
                O[f, :, at] = O[f, :, at] + tend[:, i * LANES : (i + 1) * LANES].reshape(cols, 8, LANES)

    sums = jnp.sum(Y[:, share:], axis=0) + jnp.sum(YP[:, share:], axis=0)
    cells = float(levels * east * north)
    value = jnp.broadcast_to(jnp.sqrt(jnp.maximum(sums / cells, 0.0)), (8, LANES))
    row8 = iota((8, LANES), 0)
    log = value
    for s in range(1, ITERS):
        log = jnp.where(row8 == s, pltpu.roll(value, LANES - s * fields, 1), log)
    log_ref[...] = log

    both_ends(U.at[:, pl.ds(0, 2 * HALO), body_rows], EDGE).wait_send()
    both_ends(PX, PAIR).wait_send()
    both_ends(XB.at[pl.ds(0, chips - 1)], SHARE).wait_send()
    both_ends(Y.at[pl.ds(0, chips - 1)], ALL).wait_send()
    both_ends(YP, BACK).wait_send()


def writer(O, log_ref, o_hbm, res_ref, sem):
    fields, cols, levels, north = o_hbm.shape
    chunks = north // LANES
    o_view = O.reshape(fields, cols, chunks, levels, LANES)
    for t in range(chunks):
        pltpu.make_async_copy(
            o_view.at[:, :, t], o_hbm.at[:, :, :, pl.ds(t * LANES, LANES)], sem
        ).start()
    res_ref[...] = log_ref[: res_ref.shape[0], : res_ref.shape[1]]
    pltpu.make_async_copy(O, O, sem).wait()


def solution(mesh):
    tiles = mesh.shape["gx"]
    chips = tiles // CORES

    def local(model_state, driving, mode_east, mode_north, level_class, nudge_table):
        fields, levels, cols, north = model_state.shape
        rows = levels * north // LANES
        wide, high_rows = cols + 2 * HALO, rows + 2 * PAD
        share = 16 * levels // chips
        vm = lambda *shape: pltpu.VMEM(shape, F32)
        dma = lambda *shape: pltpu.SemaphoreType.DMA(shape)
        hbm = pl.BlockSpec(memory_space=pltpu.HBM)
        smem = lambda ref: pltpu.SMEM(ref.shape, ref.dtype)
        table = nudge_table.T
        scratch = [
            smem(mode_east), smem(mode_north), smem(level_class), smem(table),
            vm(fields, wide, high_rows, LANES), vm(fields, cols, rows, LANES),
            vm(fields, ITERS - 1, wide, high_rows, LANES), pltpu.VMEM((LANES, north), jnp.bfloat16),
            vm(CORES, 32 * levels, LANES), vm(32 * levels, LANES),
            vm(chips, 2 * share, LANES), vm(chips, 2 * share, LANES),
            vm(chips, share + 1, LANES), vm(chips, share + 1, LANES), vm(CORES, 16 * levels, LANES),
            vm(ITERS * fields, 8, LANES), pltpu.VMEM((fields, 8 * cols, 2 * LANES), jnp.bfloat16),
            dma(4), dma(2, fields // 2), dma(2, fields), dma(2, 5), pltpu.SemaphoreType.REGULAR((4,)),
        ]
        turn = (0, 2, 1, 3)
        inner = pl.BlockSpec(memory_space=pltpu.VMEM)
        grid, log = pl.pallas_call(
            functools.partial(kernel, tiles),
            out_shape=(
                vm(fields, cols, rows, LANES),
                vm(8, LANES),
            ),
            in_specs=[hbm] * 6,
            out_specs=(inner, inner),
            scratch_shapes=scratch,
            compiler_params=pltpu.CompilerParams(
                collective_id=0, has_side_effects=True, vmem_limit_bytes=60 * 2**20
            ),
        )(
            model_state.transpose(turn), driving.transpose(turn),
            mode_east, mode_north, level_class, table,
        )
        nudged, log = pl.pallas_call(
            writer,
            out_shape=(
                jax.ShapeDtypeStruct((fields, cols, levels, north), F32),
                jax.ShapeDtypeStruct((ITERS, fields), F32),
            ),
            in_specs=[inner, inner],
            out_specs=(hbm, inner),
            scratch_shapes=[pltpu.SemaphoreType.DMA],
            compiler_params=pltpu.CompilerParams(vmem_limit_bytes=8 * 2**20),
        )(grid, log)
        return nudged.transpose(turn), log

    tile = P("ens", None, "gx", None)
    return jax.shard_map(
        local, mesh=mesh, in_specs=(tile, tile, P(), P(), P(), P()),
        out_specs=(tile, P("ens", None)), check_vma=False,
    )
```
